8 devices in a mesh: dp: 8 (over z, y, x, core).
Axes of the slice: x: 2, y: 2, z: 1, core: 2. Of those that a mesh axis runs over, the one named last changes fastest.
Arguments:
- act_in: bfloat16 [2048, 7, 7, 512], P('dp')
- shortcut: bfloat16 [2048, 7, 7, 2048], P('dp')
- labels: int32 [2048], P('dp')
- w_conv: float32 [512, 2048], replicated
- bn_gamma: float32 [2048], replicated
- bn_beta: float32 [2048], replicated
- w_fc: float32 [2048, 21843], replicated
- fc_bias: float32 [21843], replicated
- vel_conv: float32 [512, 2048], replicated
- vel_gamma: float32 [2048], replicated
- vel_beta: float32 [2048], replicated
- vel_fc: float32 [2048, 21843], replicated
- vel_bias: float32 [21843], replicated
- learn_rate: float32 [], replicated
Outputs:
- output 1: float32 [512, 2048], replicated
- output 2: float32 [2048], replicated
- output 3: float32 [2048], replicated
- output 4: float32 [2048, 21843], replicated
- output 5: float32 [21843], replicated
- output 6: float32 [512, 2048], replicated
- output 7: float32 [2048], replicated
- output 8: float32 [2048], replicated
- output 9: float32 [2048, 21843], replicated
- output 10: float32 [21843], replicated
- output 11: float32 [], replicated
All inputs are finite; a program needn't handle non-finite values.
Results may differ from the reference program's by a relative error of at most 0.00856896.
Values sent between devices are 32-bit elements.
A program may use at most 3 GiB of HBM per device.

```python
import jax
import jax.numpy as jnp
from jax import lax

B_DEV = 256
DP = 8
SIDE = 7
C_MID = 512
C_OUT = 2048
CLASSES = 21843

BN_EPS = 1e-5
SMOOTHING = 0.1
MOMENTUM = 0.9
TRUST_COEF = 0.001
WEIGHT_DECAY = 5e-5


def setup_inputs(seed: int = 0) -> dict:
    root_key = jax.random.key(seed)
    sub_keys = jax.random.split(root_key, 16)
    global_rows = DP * B_DEV
    step_scale = 2.5
    dev_shift = 0.5 * jax.random.normal(sub_keys[0], (DP, 1, 1, 1, C_MID), jnp.float32)
    act_in = jax.nn.relu(jax.random.normal(sub_keys[1], (DP, B_DEV, SIDE, SIDE, C_MID), jnp.float32) + dev_shift)
    act_in = act_in.reshape(global_rows, SIDE, SIDE, C_MID).astype(jnp.bfloat16)
    shortcut = jax.nn.relu(jax.random.normal(sub_keys[2], (global_rows, SIDE, SIDE, C_OUT), jnp.float32)).astype(jnp.bfloat16)
    labels = jax.random.randint(sub_keys[3], (global_rows,), 0, CLASSES, jnp.int32)
    w_conv = C_MID ** -0.5 * jax.random.normal(sub_keys[4], (C_MID, C_OUT), jnp.float32)
    bn_gamma = jax.random.uniform(sub_keys[5], (C_OUT,), jnp.float32, 0.5, 1.5)
    bn_beta = 0.5 * jax.random.normal(sub_keys[6], (C_OUT,), jnp.float32)
    w_fc = C_OUT ** -0.5 * jax.random.normal(sub_keys[7], (C_OUT, CLASSES), jnp.float32)
    fc_bias = 0.5 * jax.random.normal(sub_keys[8], (CLASSES,), jnp.float32)
    vel_conv = 0.001 * step_scale * C_MID ** -0.5 * jax.random.normal(sub_keys[9], (C_MID, C_OUT), jnp.float32)
    vel_gamma = 0.5 * step_scale * (global_rows * C_OUT) ** -0.5 * jax.random.normal(sub_keys[10], (C_OUT,), jnp.float32)
    vel_beta = 0.5 * step_scale * (global_rows * C_OUT) ** -0.5 * jax.random.normal(sub_keys[11], (C_OUT,), jnp.float32)
    vel_fc = 0.001 * step_scale * C_OUT ** -0.5 * jax.random.normal(sub_keys[12], (C_OUT, CLASSES), jnp.float32)
    vel_bias = 0.9 * step_scale * (global_rows * CLASSES) ** -0.5 * jax.random.normal(sub_keys[13], (CLASSES,), jnp.float32)
    learn_rate = jax.random.uniform(sub_keys[14], (), jnp.float32, 1.0, 4.0)
    return {'act_in': act_in, 'shortcut': shortcut, 'labels': labels, 'w_conv': w_conv, 'bn_gamma': bn_gamma, 'bn_beta': bn_beta, 'w_fc': w_fc, 'fc_bias': fc_bias, 'vel_conv': vel_conv, 'vel_gamma': vel_gamma, 'vel_beta': vel_beta, 'vel_fc': vel_fc, 'vel_bias': vel_bias, 'learn_rate': learn_rate}


def group_loss(params, act_grp, short_grp, label_grp):
    w_conv, bn_gamma, bn_beta, w_fc, fc_bias = params
    pos_count = B_DEV * SIDE * SIDE
    conv_out = jnp.dot(act_grp.reshape(pos_count, C_MID), w_conv.astype(jnp.bfloat16), preferred_element_type=jnp.float32)
    batch_mean = jnp.mean(conv_out, axis=0)
    centered = conv_out - batch_mean
    batch_var = jnp.mean(jnp.square(centered), axis=0)
    x_hat = centered * lax.rsqrt(batch_var + BN_EPS)
    activ = jax.nn.relu(x_hat * bn_gamma + bn_beta + short_grp.reshape(pos_count, C_OUT).astype(jnp.float32))
    pooled = jnp.mean(activ.reshape(B_DEV, SIDE * SIDE, C_OUT), axis=1)
    logits = jnp.dot(pooled.astype(jnp.bfloat16), w_fc.astype(jnp.bfloat16), preferred_element_type=jnp.float32) + fc_bias
    log_prob = jax.nn.log_softmax(logits, axis=-1)
    one_hot_lab = (label_grp[:, None] == jnp.arange(CLASSES)[None, :]).astype(jnp.float32)
    target = SMOOTHING / CLASSES + (1.0 - SMOOTHING) * one_hot_lab
    return -jnp.sum(target * log_prob)


def lars_update(weight, gradient, velocity, learn_rate):
    w_norm = jnp.sqrt(jnp.sum(jnp.square(weight)))
    g_norm = jnp.sqrt(jnp.sum(jnp.square(gradient)))
    trust = TRUST_COEF * w_norm / (g_norm + WEIGHT_DECAY * w_norm)
    new_vel = MOMENTUM * velocity + learn_rate * trust * (gradient + WEIGHT_DECAY * weight)
    return weight - new_vel, new_vel


def reference(act_in, shortcut, labels, w_conv, bn_gamma, bn_beta, w_fc, fc_bias, vel_conv, vel_gamma, vel_beta, vel_fc, vel_bias, learn_rate):
    params = (w_conv, bn_gamma, bn_beta, w_fc, fc_bias)
    grad_fn = jax.value_and_grad(group_loss)
    global_rows = DP * B_DEV

    def scan_body(carry, group_batch):
        loss_sum, grad_sum = carry
        loss_val, grads = grad_fn(params, group_batch[0], group_batch[1], group_batch[2])
        return (loss_sum + loss_val, jax.tree.map(jnp.add, grad_sum, grads)), None

    init_carry = (jnp.zeros((), jnp.float32), jax.tree.map(jnp.zeros_like, params))
    group_data = (act_in.reshape(DP, B_DEV, SIDE, SIDE, C_MID), shortcut.reshape(DP, B_DEV, SIDE, SIDE, C_OUT), labels.reshape(DP, B_DEV))
    (loss_sum, grad_sum), unused_out = lax.scan(scan_body, init_carry, group_data)
    g_conv, g_gamma, g_beta, g_fc, g_bias = [grad_part / global_rows for grad_part in grad_sum]
    conv_new, conv_vel_new = lars_update(w_conv, g_conv, vel_conv, learn_rate)
    fc_new, fc_vel_new = lars_update(w_fc, g_fc, vel_fc, learn_rate)
    gamma_vel_new = MOMENTUM * vel_gamma + learn_rate * g_gamma
    beta_vel_new = MOMENTUM * vel_beta + learn_rate * g_beta
    bias_vel_new = MOMENTUM * vel_bias + learn_rate * g_bias
    return (conv_new, bn_gamma - gamma_vel_new, bn_beta - beta_vel_new, fc_new, fc_bias - bias_vel_new, conv_vel_new, gamma_vel_new, beta_vel_new, fc_vel_new, bias_vel_new, loss_sum / global_rows)
```

```python
import functools

import jax
import jax.numpy as jnp
from jax import lax
from jax.experimental import pallas as pl
from jax.experimental.pallas import tpu as pltpu
from jax.sharding import PartitionSpec as P

BN_EPS = 1e-5
SMOOTHING = 0.1
MOMENTUM = 0.9
TRUST_COEF = 0.001
WEIGHT_DECAY = 5e-5

TILE = 256
BLK = 32
SLOTS = TILE // BLK
HAVE = 3
NORM = 2
GROUP = 3
CHUNK = 512
VMEM_LIMIT = 66_000_000


def tiled(x, reps):
    return jnp.concatenate([x] * reps, axis=1)


def logit_grads(z, bias, lse, lab, base, classes):
    cols = z.shape[1]
    row = lax.broadcasted_iota(jnp.int32, (BLK, cols), 0) + base
    e = jnp.exp(z + tiled(bias, cols // 128) - lse)
    low = SMOOTHING / classes
    return e - jnp.where(lab == row, low + (1.0 - SMOOTHING), low)


def grad_kernel(classes, rows_total, sc, *refs):
    nw = GROUP * HAVE
    ws, biases = refs[:nw], refs[nw:nw + GROUP]
    pt, p, lse, lab, g_out, db_out, sq_out, lhs, dmat = refs[nw + GROUP:]
    q, c = sc[0], sc[1]
    step = pl.program_id(0)
    cols = pt.shape[1]
    feats = pt.shape[0]

    @pl.when(step == 0)
    def _():
        sq_out[...] = jnp.zeros_like(sq_out)

    bases, slots = [], []
    for t in range(GROUP):
        tile = 2 * (GROUP * step + t) + c
        for i in range(HAVE):
            slot = lax.rem(2 * q + i, SLOTS)
            slots.append(slot)
            bases.append(tile * TILE + slot * BLK)
    for k in range(nw):
        valid = lax.broadcasted_iota(jnp.int32, (BLK, feats), 0) < classes - bases[k]
        w = jnp.where(valid, ws[k][...], 0.0)
        if k % HAVE < NORM:
            sq_out[1] += jnp.sum((w * w).reshape(BLK // 8, 8, feats), axis=0)
        lhs[k * BLK:(k + 1) * BLK, :] = w.astype(jnp.bfloat16)
    sums = [jnp.zeros((BLK, 128), jnp.float32) for _ in range(nw)]
    for n in range(cols // CHUNK):
        cs = slice(n * CHUNK, (n + 1) * CHUNK)
        z = jnp.dot(lhs[...], pt[:, cs], preferred_element_type=jnp.float32)
        for k in range(nw):
            rs = slice(k * BLK, (k + 1) * BLK)
            bias = biases[k // HAVE][pl.ds(pl.multiple_of(slots[k] * BLK, BLK), BLK), :]
            d = logit_grads(z[rs], bias, lse[:, cs], lab[:, cs], bases[k], classes)
            valid = lax.broadcasted_iota(jnp.int32, (BLK, CHUNK), 0) < classes - bases[k]
            d = jnp.where(valid, d, 0.0)
            for m in range(CHUNK // 128):
                sums[k] = sums[k] + d[:, m * 128:(m + 1) * 128]
            dmat[rs, cs] = d.astype(jnp.bfloat16)
    for k in range(nw):
        db_out[k // HAVE, (k % HAVE) * BLK:(k % HAVE + 1) * BLK, :] = sums[k]
    for n in range(feats // CHUNK):
        cs = slice(n * CHUNK, (n + 1) * CHUNK)
        g = jnp.dot(dmat[...], p[:, cs], preferred_element_type=jnp.float32) * (1.0 / rows_total)
        for k in range(nw):
            gk = g[k * BLK:(k + 1) * BLK]
            g_out[k // HAVE, (k % HAVE) * BLK:(k % HAVE + 1) * BLK, cs] = gk
            if k % HAVE < NORM:
                sq_out[0, :, cs] += jnp.sum((gk * gk).reshape(BLK // 8, 8, CHUNK), axis=0)


def shared_grads(sc, wt, bias, pt, p, lse, lab):
    classes, feats = wt.shape
    rows_total = p.shape[0]
    n_tiles = pl.cdiv(classes, TILE)
    steps = pl.cdiv(pl.cdiv(n_tiles, 2), GROUP)
    last = pl.cdiv(classes, BLK) - 1

    def w_map(t, i):
        return lambda s, sc: (jnp.minimum((2 * (GROUP * s + t) + sc[1]) * SLOTS + lax.rem(2 * sc[0] + i, SLOTS), last), 0)

    def b_map(t):
        return lambda s, sc: (jnp.minimum(2 * (GROUP * s + t) + sc[1], n_tiles - 1), 0)

    once = dict(pipeline_mode=pl.Buffered(1))
    whole = lambda a: pl.BlockSpec(a.shape, lambda s, sc: (0, 0), **once)
    rows = GROUP * HAVE * BLK
    return pl.pallas_call(
        functools.partial(grad_kernel, classes, rows_total),
        grid_spec=pltpu.PrefetchScalarGridSpec(
            num_scalar_prefetch=1,
            grid=(steps,),
            in_specs=[pl.BlockSpec((BLK, feats), w_map(t, i)) for t in range(GROUP) for i in range(HAVE)]
            + [pl.BlockSpec((TILE, 128), b_map(t)) for t in range(GROUP)]
            + [whole(pt), whole(p), whole(lse), whole(lab)],
            out_specs=[
                pl.BlockSpec((GROUP, HAVE * BLK, feats), lambda s, sc: (s, 0, 0)),
                pl.BlockSpec((GROUP, HAVE * BLK, 128), lambda s, sc: (s, 0, 0)),
                pl.BlockSpec((2, 8, feats), lambda s, sc: (0, 0, 0)),
            ],
            scratch_shapes=[pltpu.VMEM((rows, feats), jnp.bfloat16), pltpu.VMEM((rows, rows_total), jnp.bfloat16)],
        ),
        out_shape=[
            jax.ShapeDtypeStruct((steps * GROUP, HAVE * BLK, feats), jnp.float32),
            jax.ShapeDtypeStruct((steps * GROUP, HAVE * BLK, 128), jnp.float32),
            jax.ShapeDtypeStruct((2, 8, feats), jnp.float32),
        ],
        compiler_params=pltpu.CompilerParams(dimension_semantics=("arbitrary",), vmem_limit_bytes=VMEM_LIMIT),
        cost_estimate=pl.CostEstimate(flops=4 * steps * rows * feats * rows_total, bytes_accessed=8 * steps * rows * feats, transcendentals=0),
        name="shared_grads",
    )(sc, *([wt] * (GROUP * HAVE)), *([bias] * GROUP), pt, p, lse, lab)


def update_kernel(classes, rows_total, sc, rate, w_in, v_in, own, other, bias, pt, p, lse, lab, w_out, v_out, lhs, dmat):
    q, c = sc[0], sc[1]
    step = pl.program_id(0)
    a = rate[0]
    cols = pt.shape[1]
    feats = pt.shape[0]

    def rows_at(base):
        return pl.ds(pl.multiple_of(base, BLK), BLK)

    def apply(rs, cs, g):
        w = w_in[rs, cs]
        nv = MOMENTUM * v_in[rs, cs] + a * (g + WEIGHT_DECAY * w)
        v_out[rs, cs] = nv
        w_out[rs, cs] = w - nv

    bases = []
    for t in range(2):
        for i in range(HAVE, SLOTS):
            bases.append(t * TILE + lax.rem(2 * q + i, SLOTS) * BLK)
    for k, base in enumerate(bases):
        lhs[k * BLK:(k + 1) * BLK, :] = w_in[rows_at(base), :].astype(jnp.bfloat16)
    known = []
    for src, t in ((own, c), (other, 1 - c)):
        for i in range(HAVE):
            known.append((src, i, t * TILE + lax.rem(2 * q + i, SLOTS) * BLK))
    for n in range(cols // CHUNK):
        cs = slice(n * CHUNK, (n + 1) * CHUNK)
        z = jnp.dot(lhs[...], pt[:, cs], preferred_element_type=jnp.float32)
        for src, i, base in known:
            apply(rows_at(base), cs, src[0, i * BLK:(i + 1) * BLK, cs])
        for k, base in enumerate(bases):
            rs = slice(k * BLK, (k + 1) * BLK)
            d = logit_grads(z[rs], bias[rows_at(base), :], lse[:, cs], lab[:, cs], step * 2 * TILE + base, classes)
            dmat[rs, cs] = d.astype(jnp.bfloat16)
    for n in range(feats // CHUNK):
        cs = slice(n * CHUNK, (n + 1) * CHUNK)
        g = jnp.dot(dmat[...], p[:, cs], preferred_element_type=jnp.float32) * (1.0 / rows_total)
        for k, base in enumerate(bases):
            apply(rows_at(base), cs, g[k * BLK:(k + 1) * BLK])


def fused_update(sc, rate, wt, vt, own, other, bias, pt, p, lse, lab):
    classes, feats = wt.shape
    rows_total = p.shape[0]
    steps = pl.cdiv(classes, 2 * TILE)
    once = dict(pipeline_mode=pl.Buffered(1))
    whole = lambda a: pl.BlockSpec(a.shape, lambda s, sc: (0, 0), **once)
    tile = pl.BlockSpec((2 * TILE, feats), lambda s, sc: (s, 0))
    part = pl.BlockSpec((1, HAVE * BLK, feats), lambda s, sc: (s, 0, 0))
    rows = 2 * (SLOTS - HAVE) * BLK
    return pl.pallas_call(
        functools.partial(update_kernel, classes, rows_total),
        grid_spec=pltpu.PrefetchScalarGridSpec(
            num_scalar_prefetch=1,
            grid=(steps,),
            in_specs=[pl.BlockSpec(memory_space=pltpu.SMEM), tile, tile, part, part,
                      pl.BlockSpec((2 * TILE, 128), lambda s, sc: (s, 0)),
                      whole(pt), whole(p), whole(lse), whole(lab)],
            out_specs=[tile, tile],
            scratch_shapes=[pltpu.VMEM((rows, feats), jnp.bfloat16), pltpu.VMEM((rows, rows_total), jnp.bfloat16)],
        ),
        out_shape=[jax.ShapeDtypeStruct(wt.shape, jnp.float32)] * 2,
        compiler_params=pltpu.CompilerParams(dimension_semantics=("arbitrary",), vmem_limit_bytes=VMEM_LIMIT),
        cost_estimate=pl.CostEstimate(flops=4 * steps * rows * feats * rows_total, bytes_accessed=16 * classes * feats, transcendentals=0),
        name="fused_update",
    )(sc, rate, wt, vt, own, other, bias, pt, p, lse, lab)


def round_kernel(x, p, pt):
    r = x[...].astype(jnp.bfloat16)
    p[...] = r
    pt[...] = r.T


def round_both(x):
    n, m = x.shape
    return pl.pallas_call(
        round_kernel,
        grid=(n // TILE,),
        in_specs=[pl.BlockSpec((TILE, m), lambda i: (i, 0))],
        out_specs=[pl.BlockSpec((TILE, m), lambda i: (i, 0)), pl.BlockSpec((m, TILE), lambda i: (0, i))],
        out_shape=[jax.ShapeDtypeStruct((n, m), jnp.bfloat16), jax.ShapeDtypeStruct((m, n), jnp.bfloat16)],
        compiler_params=pltpu.CompilerParams(dimension_semantics=("arbitrary",)),
        cost_estimate=pl.CostEstimate(flops=2 * n * m, bytes_accessed=8 * n * m, transcendentals=0),
        name="round_both",
    )(x)


def solution(mesh):
    groups = mesh.shape['dp']
    swap = [(i, i ^ 1) for i in range(groups)]

    def local_step(act_in, shortcut, labels, w_conv, bn_gamma, bn_beta, w_fc, fc_bias, vel_conv, vel_gamma, vel_beta, vel_fc, vel_bias, learn_rate):
        per_dev = act_in.shape[0]
        global_rows = per_dev * groups
        spatial = act_in.shape[1] * act_in.shape[2]
        c_mid = act_in.shape[3]
        c_out = shortcut.shape[3]
        classes = w_fc.shape[1]
        pos_count = per_dev * spatial
        dev = lax.axis_index('dp')
        sc = jnp.stack([dev // 2, dev % 2]).astype(jnp.int32)
        act_grid = act_in.reshape(per_dev, spatial, c_mid)
        conv_out = jnp.einsum('bpc,cd->bpd', act_grid, w_conv.astype(jnp.bfloat16), preferred_element_type=jnp.float32)
        batch_mean = jnp.mean(conv_out, axis=(0, 1))
        centered = conv_out - batch_mean
        inv_std = lax.rsqrt(jnp.mean(jnp.square(centered), axis=(0, 1)) + BN_EPS)
        x_hat = centered * inv_std
        pre_act = x_hat * bn_gamma + bn_beta + shortcut.reshape(per_dev, spatial, c_out).astype(jnp.float32)
        pooled = jnp.mean(jax.nn.relu(pre_act), axis=1)
        pooled_bf = pooled.astype(jnp.bfloat16)
        p_all = lax.all_gather(pooled, 'dp', tiled=True)
        fc_bf = w_fc.astype(jnp.bfloat16)
        logits = jnp.dot(pooled_bf, fc_bf, preferred_element_type=jnp.float32) + fc_bias
        top = jnp.max(logits, axis=-1, keepdims=True)
        lse = top + jnp.log(jnp.sum(jnp.exp(logits - top), axis=-1, keepdims=True))
        one_hot_lab = (labels[:, None] == jnp.arange(classes, dtype=jnp.int32)[None, :]).astype(jnp.float32)
        target = SMOOTHING / classes + (1.0 - SMOOTHING) * one_hot_lab
        log_prob = logits - lse
        loss_part = -jnp.sum(target * log_prob) / global_rows
        d_logits_bf = (jnp.exp(log_prob) - target).astype(jnp.bfloat16)
        d_pool = jnp.einsum('bk,ck->bc', d_logits_bf, fc_bf, preferred_element_type=jnp.float32) / (spatial * global_rows)
        d_pre = jnp.where(pre_act > 0, d_pool[:, None, :], 0.0)
        d_beta = jnp.sum(d_pre, axis=(0, 1))
        d_gamma = jnp.sum(d_pre * x_hat, axis=(0, 1))
        d_conv_out = (bn_gamma * inv_std) * (d_pre - d_beta / pos_count - x_hat * (d_gamma / pos_count))
        d_conv = jnp.einsum('bpc,bpd->cd', act_grid, d_conv_out.astype(jnp.bfloat16), preferred_element_type=jnp.float32)

        small = lax.all_gather(jnp.concatenate([lse, labels[:, None].astype(jnp.float32)], axis=1), 'dp', tiled=True)
        lse_all = small[:, 0][None, :]
        lab_all = small[:, 1].astype(jnp.int32)[None, :]
        p_bf, pt_bf = round_both(p_all)
        wt, vt = w_fc.T, vel_fc.T
        n_tiles = pl.cdiv(classes, TILE)
        bias_wide = jnp.broadcast_to(jnp.pad(fc_bias, (0, n_tiles * TILE - classes))[:, None], (n_tiles * TILE, 128))
        own, db, sq = shared_grads(sc, wt, bias_wide, pt_bf, p_bf, lse_all, lab_all)
        other = lax.ppermute(own, 'dp', swap)
        sq = jnp.sum(sq, axis=(1, 2))
        half = pl.cdiv(n_tiles, 2)
        db = jnp.sum(db[:half, :NORM * BLK], axis=-1) / global_rows
        d_bias = lax.dynamic_update_slice(jnp.zeros((half, 2, TILE), jnp.float32), db[:, None, :], (0, sc[1], sc[0] * NORM * BLK))
        d_bias = d_bias.reshape(-1)[:classes]
        sq, g_gamma, g_beta, loss_val = lax.psum((sq, d_gamma, d_beta, loss_part), 'dp')
        g_conv, g_bias = lax.psum((d_conv, d_bias), 'dp')
        g_norm, w_norm = jnp.sqrt(sq[0]), jnp.sqrt(sq[1])
        rate = learn_rate * TRUST_COEF * w_norm / (g_norm + WEIGHT_DECAY * w_norm)
        fc_new, fc_vel_new = fused_update(sc, rate[None], wt, vt, own, other, bias_wide, pt_bf, p_bf, lse_all, lab_all)
        cw = jnp.sqrt(jnp.sum(jnp.square(w_conv)))
        cg = jnp.sqrt(jnp.sum(jnp.square(g_conv)))
        trust = TRUST_COEF * cw / (cg + WEIGHT_DECAY * cw)
        conv_vel_new = MOMENTUM * vel_conv + learn_rate * trust * (g_conv + WEIGHT_DECAY * w_conv)
        gamma_vel_new = MOMENTUM * vel_gamma + learn_rate * g_gamma
        beta_vel_new = MOMENTUM * vel_beta + learn_rate * g_beta
        bias_vel_new = MOMENTUM * vel_bias + learn_rate * g_bias
        return (w_conv - conv_vel_new, bn_gamma - gamma_vel_new, bn_beta - beta_vel_new, fc_new.T, fc_bias - bias_vel_new, conv_vel_new, gamma_vel_new, beta_vel_new, fc_vel_new.T, bias_vel_new, loss_val)

    return jax.shard_map(local_step, mesh=mesh, in_specs=(P('dp'),) * 3 + (P(),) * 11, out_specs=(P(),) * 11, check_vma=False)
```

```python
import functools

import jax
import jax.numpy as jnp
from jax import lax
from jax.experimental import pallas as pl
from jax.experimental.pallas import tpu as pltpu
from jax.sharding import PartitionSpec as P

BN_EPS = 1e-5
SMOOTHING = 0.1
MOMENTUM = 0.9
TRUST_COEF = 0.001
WEIGHT_DECAY = 5e-5

TILE = 256
BLK = 32
SLOTS = TILE // BLK
HAVE = 3
NORM = 2
GROUP = 3
CHUNK = 512
POS = 7
WIDTH = 512
LANES = 128
SUB = 8
RING = 4
VMEM_LIMIT = 66_000_000


def aligned(i, size):
    return pl.ds(pl.multiple_of(i, size), size)


def tiled(x, reps):
    return jnp.concatenate([x] * reps, axis=1)


def logit_grads(z, bias, lse, lab, base, classes):
    cols = z.shape[1]
    row = (lax.broadcasted_iota(jnp.int32, (BLK, cols), 0) + base).astype(jnp.float32)
    e = jnp.exp(z + tiled(bias, cols // LANES) - lse)
    low = SMOOTHING / classes
    return e - jnp.where(lab == row, low + (1.0 - SMOOTHING), low)


def grad_kernel(classes, groups, steps, *refs):
    nw = GROUP * HAVE
    ws, biases = refs[:nw], refs[nw:nw + GROUP]
    (p_all, own, lr, g_out, p_out, db_out, rows_out, rate_out, p, pbuf, lhs, dmat, gbuf, meta, sq, msg, msgs,
     p_sem, keep_sem, g_sem, gs_sem, gr_sem, meta_s, meta_r, msg_s, msg_r) = refs[nw + GROUP:]
    me = lax.axis_index('dp')
    q, c = me // 2, me % 2
    step = pl.program_id(0)
    rows_total, feats = p.shape
    per_dev = rows_total // groups

    def slot_of(i):
        return (2 * q + i) % SLOTS

    def base_of(group, k):
        return (2 * (GROUP * group + k // HAVE) + c) * TILE + slot_of(k % HAVE) * BLK

    def prepare(group):
        for k in range(nw):
            valid = lax.broadcasted_iota(jnp.int32, (BLK, feats), 0) < classes - base_of(group, k)
            w = jnp.where(valid, ws[k][...], 0.0)
            if k % HAVE < NORM:
                sq[1] += jnp.sum((w * w).reshape(BLK // 8, 8, feats), axis=0)
            lhs[group % 2, k * BLK:(k + 1) * BLK, :] = w.astype(jnp.bfloat16)

    def local(group):
        return pltpu.make_async_copy(gbuf.at[group % 2], g_out.at[c, pl.ds(group * GROUP, GROUP)], g_sem.at[group % 2])

    def remote(group):
        return pltpu.make_async_remote_copy(
            gbuf.at[group % 2], g_out.at[c, pl.ds(group * GROUP, GROUP)], gs_sem.at[group % 2], gr_sem.at[group],
            device_id=(me + 1 - 2 * c,), device_id_type=pl.DeviceIdType.MESH)

    def arrival(group):
        return pltpu.make_async_remote_copy(
            gbuf.at[group % 2], g_out.at[1 - c, pl.ds(group * GROUP, GROUP)], gs_sem.at[group % 2], gr_sem.at[group],
            device_id=(me + 1 - 2 * c,), device_id_type=pl.DeviceIdType.MESH)

    def spread(src, dst, send, recv):
        return [pltpu.make_async_remote_copy(
            src, dst.at[me], send.at[o], recv.at[o],
            device_id=((me + o) % groups,), device_id_type=pl.DeviceIdType.MESH) for o in range(1, groups)]

    keep = pltpu.make_async_copy(p, p_out, keep_sem)

    @pl.when(step == 0)
    def _():
        def fetch(i, slot):
            return pltpu.make_async_copy(p_all.at[aligned(i * per_dev, per_dev)], pbuf.at[slot], p_sem.at[slot])

        fetch(0, 0).start()
        barrier = pltpu.get_barrier_semaphore()
        for o in range(1, groups):
            pl.semaphore_signal(barrier, 1, device_id=((me + o) % groups,), device_id_type=pl.DeviceIdType.MESH)
        pl.semaphore_wait(barrier, groups - 1)
        for copy in spread(own, meta, meta_s, meta_r):
            copy.start()
        meta[me] = own[...]
        sq[...] = jnp.zeros_like(sq)
        prepare(0)

        def convert(i, carry):
            @pl.when(i + 1 < groups)
            def _():
                fetch(i + 1, (i + 1) % 2).start()
            fetch(i, i % 2).wait()
            at = aligned(i * per_dev, per_dev)
            p[at, :] = pbuf[i % 2].astype(jnp.bfloat16)
            return carry

        lax.fori_loop(0, groups, convert, 0)
        keep.start()
        for copy in spread(own, meta, meta_s, meta_r):
            copy.wait()
        for d in range(groups):
            rows_out[:, d * per_dev:(d + 1) * per_dev] = meta[d]

    @pl.when(step > 1)
    def _():
        local(step - 2).start()
        remote(step - 2).start()

    @pl.when(step > 2)
    def _():
        local(step - 3).wait()
        remote(step - 3).wait_send()

    @pl.when(step > 0)
    def _():
        group = step - 1
        now = group % 2
        prepare(step)
        sums = [jnp.zeros((BLK, LANES), jnp.float32) for _ in range(nw)]
        for n in range(rows_total // CHUNK):
            cs = slice(n * CHUNK, (n + 1) * CHUNK)
            z = lax.dot_general(lhs[now], p[cs, :], (((1,), (1,)), ((), ())), preferred_element_type=jnp.float32)
            for k in range(nw):
                rs = slice(k * BLK, (k + 1) * BLK)
                bias = biases[k // HAVE][aligned(slot_of(k % HAVE) * BLK, BLK), :]
                d = logit_grads(z[rs], bias, rows_out[0:1, cs], rows_out[1:2, cs], base_of(group, k), classes)
                valid = lax.broadcasted_iota(jnp.int32, (BLK, CHUNK), 0) < classes - base_of(group, k)
                d = jnp.where(valid, d, 0.0)
                for m in range(CHUNK // LANES):
                    sums[k] = sums[k] + d[:, m * LANES:(m + 1) * LANES]
                dmat[rs, cs] = d.astype(jnp.bfloat16)
        for k in range(nw):
            db_out[k // HAVE, (k % HAVE) * BLK:(k % HAVE + 1) * BLK, :] = sums[k]
        for n in range(feats // CHUNK):
            cs = slice(n * CHUNK, (n + 1) * CHUNK)
            g = jnp.dot(dmat[...], p[:, cs], preferred_element_type=jnp.float32) * (1.0 / rows_total)
            for k in range(nw):
                gk = g[k * BLK:(k + 1) * BLK]
                gbuf[now, k // HAVE, (k % HAVE) * BLK:(k % HAVE + 1) * BLK, cs] = gk
                if k % HAVE < NORM:
                    sq[0, :, cs] += jnp.sum((gk * gk).reshape(BLK // 8, 8, CHUNK), axis=0)

    @pl.when(step == steps)
    def _():
        for i in range(2):
            parts = sq[i]
            total = parts[:, 0:LANES]
            for m in range(1, feats // LANES):
                total = total + parts[:, m * LANES:(m + 1) * LANES]
            msg[i] = total
        local(steps - 1).start()
        remote(steps - 1).start()
        for group in (steps - 2, steps - 1):
            local(group).wait()
            remote(group).wait_send()
        keep.wait()
        for copy in spread(msg, msgs, msg_s, msg_r):
            copy.start()
        msgs[me] = msg[...]
        for group in range(steps):
            arrival(group).wait_recv()
        for copy in spread(msg, msgs, msg_s, msg_r):
            copy.wait()
        both = jnp.sum(msgs[...], axis=0)
        g_norm = jnp.sqrt(jnp.sum(both[0]))
        w_norm = jnp.sqrt(jnp.sum(both[1]))
        rate_out[...] = jnp.full(rate_out.shape, lr[0] * TRUST_COEF * w_norm / (g_norm + WEIGHT_DECAY * w_norm), jnp.float32)


def shared_grads(groups, wt, bias, p_all, own, lr):
    classes, feats = wt.shape
    rows_total = p_all.shape[0]
    n_tiles = pl.cdiv(classes, TILE)
    steps = pl.cdiv(pl.cdiv(n_tiles, 2), GROUP)
    last = pl.cdiv(classes, BLK) - 1

    def w_map(t, i):
        def index(s):
            me = lax.axis_index('dp')
            tile = 2 * (GROUP * jnp.minimum(s, steps - 1) + t) + me % 2
            return jnp.minimum(tile * SLOTS + (2 * (me // 2) + i) % SLOTS, last), 0
        return index

    def b_map(t):
        return lambda s: (jnp.minimum(2 * (GROUP * jnp.maximum(s - 1, 0) + t) + lax.axis_index('dp') % 2, n_tiles - 1), 0)

    rows = GROUP * HAVE * BLK
    anywhere = pl.BlockSpec(memory_space=pl.ANY)
    dma = pltpu.SemaphoreType.DMA
    return pl.pallas_call(
        functools.partial(grad_kernel, classes, groups, steps),
        grid=(steps + 1,),
        in_specs=[pl.BlockSpec((BLK, feats), w_map(t, i)) for t in range(GROUP) for i in range(HAVE)]
        + [pl.BlockSpec((TILE, LANES), b_map(t)) for t in range(GROUP)]
        + [anywhere, pl.BlockSpec(own.shape, lambda s: (0, 0)), pl.BlockSpec(memory_space=pltpu.SMEM)],
        out_specs=[
            anywhere, anywhere,
            pl.BlockSpec((GROUP, HAVE * BLK, LANES), lambda s: (jnp.maximum(s - 1, 0), 0, 0)),
            pl.BlockSpec((8, rows_total), lambda s: (0, 0)),
            pl.BlockSpec((8, LANES), lambda s: (0, 0)),
        ],
        out_shape=[
            jax.ShapeDtypeStruct((2, steps * GROUP, HAVE * BLK, feats), jnp.float32),
            jax.ShapeDtypeStruct((rows_total, feats), jnp.bfloat16),
            jax.ShapeDtypeStruct((steps * GROUP, HAVE * BLK, LANES), jnp.float32),
            jax.ShapeDtypeStruct((8, rows_total), jnp.float32),
            jax.ShapeDtypeStruct((8, LANES), jnp.float32),
        ],
        scratch_shapes=[
            pltpu.VMEM((rows_total, feats), jnp.bfloat16),
            pltpu.VMEM((2, rows_total // groups, feats), jnp.float32),
            pltpu.VMEM((2, rows, feats), jnp.bfloat16), pltpu.VMEM((rows, rows_total), jnp.bfloat16),
            pltpu.VMEM((2, GROUP, HAVE * BLK, feats), jnp.float32),
            pltpu.VMEM((groups,) + own.shape, jnp.float32),
            pltpu.VMEM((2, 8, feats), jnp.float32), pltpu.VMEM((2, 8, LANES), jnp.float32), pltpu.VMEM((groups, 2, 8, LANES), jnp.float32),
            dma((2,)), dma, dma((2,)), dma((2,)), dma((steps,)),
            dma((groups,)), dma((groups,)), dma((groups,)), dma((groups,)),
        ],
        compiler_params=pltpu.CompilerParams(dimension_semantics=("arbitrary",), vmem_limit_bytes=VMEM_LIMIT, collective_id=0, has_side_effects=True),
        cost_estimate=pl.CostEstimate(flops=4 * steps * rows * feats * rows_total, bytes_accessed=8 * steps * rows * feats, transcendentals=0),
        name="shared_grads",
    )(*([wt] * (GROUP * HAVE)), *([bias] * GROUP), p_all, own, lr)


def update_kernel(classes, rows_total, rate, w_in, v_in, even, odd, bias, p, rows_in, w_out, v_out, done, lhs, dmat):
    q = lax.axis_index('dp') // 2
    step = pl.program_id(0)
    a = tiled(rate[0:1, :], CHUNK // LANES)
    cols, feats = p.shape
    done[...] = jnp.zeros_like(done)

    def rows_at(base):
        return aligned(base, BLK)

    def apply(rs, cs, g):
        w = w_in[rs, cs]
        nv = MOMENTUM * v_in[rs, cs] + a * (g + WEIGHT_DECAY * w)
        v_out[rs, cs] = nv
        w_out[rs, cs] = w - nv

    bases = []
    for t in range(2):
        for i in range(HAVE, SLOTS):
            bases.append(t * TILE + (2 * q + i) % SLOTS * BLK)
    for k, base in enumerate(bases):
        lhs[k * BLK:(k + 1) * BLK, :] = w_in[rows_at(base), :].astype(jnp.bfloat16)
    for n in range(cols // CHUNK):
        cs = slice(n * CHUNK, (n + 1) * CHUNK)
        z = lax.dot_general(lhs[...], p[cs, :], (((1,), (1,)), ((), ())), preferred_element_type=jnp.float32)
        for t, src in enumerate((even, odd)):
            for i in range(HAVE):
                apply(rows_at(t * TILE + (2 * q + i) % SLOTS * BLK), cs, src[0, 0, i * BLK:(i + 1) * BLK, cs])
        for k, base in enumerate(bases):
            rs = slice(k * BLK, (k + 1) * BLK)
            d = logit_grads(z[rs], bias[rows_at(base), :], rows_in[0:1, cs], rows_in[1:2, cs], step * 2 * TILE + base, classes)
            dmat[rs, cs] = d.astype(jnp.bfloat16)
    for n in range(feats // CHUNK):
        cs = slice(n * CHUNK, (n + 1) * CHUNK)
        g = jnp.dot(dmat[...], p[:, cs], preferred_element_type=jnp.float32) * (1.0 / rows_total)
        for k, base in enumerate(bases):
            apply(rows_at(base), cs, g[k * BLK:(k + 1) * BLK])


def fused_update(rate, wt, vt, grads, bias, p, rows_in):
    classes, feats = wt.shape
    rows_total = p.shape[0]
    steps = pl.cdiv(classes, 2 * TILE)
    once = dict(pipeline_mode=pl.Buffered(1))
    whole = lambda a: pl.BlockSpec(a.shape, lambda s: (0, 0), **once)
    tile = pl.BlockSpec((2 * TILE, feats), lambda s: (s, 0))
    part = lambda par: pl.BlockSpec((1, 1, HAVE * BLK, feats), lambda s: (par, s, 0, 0))
    rows = 2 * (SLOTS - HAVE) * BLK
    return pl.pallas_call(
        functools.partial(update_kernel, classes, rows_total),
        grid=(steps,),
        in_specs=[whole(rate), tile, tile, part(0), part(1), pl.BlockSpec((2 * TILE, LANES), lambda s: (s, 0)), whole(p), whole(rows_in)],
        out_specs=[tile, tile, pl.BlockSpec((8, LANES), lambda s: (0, 0))],
        scratch_shapes=[pltpu.VMEM((rows, feats), jnp.bfloat16), pltpu.VMEM((rows, rows_total), jnp.bfloat16)],
        out_shape=[jax.ShapeDtypeStruct(wt.shape, jnp.float32)] * 2 + [jax.ShapeDtypeStruct((8, LANES), jnp.float32)],
        compiler_params=pltpu.CompilerParams(dimension_semantics=("arbitrary",), vmem_limit_bytes=VMEM_LIMIT),
        cost_estimate=pl.CostEstimate(flops=4 * steps * rows * feats * rows_total, bytes_accessed=16 * classes * feats, transcendentals=0),
        name="fused_update",
    )(rate, wt, vt, grads, grads, bias, p, rows_in)


def conv_update_kernel(dep, lr, g_hbm, w_hbm, v_hbm, w_out, v_out, g, w, v, sem, out_sem):
    loads = [pltpu.make_async_copy(x, y, sem.at[i]) for i, (x, y) in enumerate(((g_hbm, g), (w_hbm, w), (v_hbm, v)))]
    for copy in loads:
        copy.start()
    parts = out_sem.shape[1]
    size = g.shape[0] // parts

    def square_sum(ref):
        def add(i, acc):
            x = ref[aligned(i * size, size)]
            return acc + jnp.sum((x * x).reshape(size // SUB, SUB, x.shape[1]), axis=0)
        return jnp.sum(lax.fori_loop(0, parts, add, jnp.zeros((SUB, ref.shape[1]), jnp.float32)))

    loads[0].wait()
    g_norm = jnp.sqrt(square_sum(g))
    loads[1].wait()
    w_norm = jnp.sqrt(square_sum(w))
    loads[2].wait()
    rate = lr[0] * TRUST_COEF * w_norm / (g_norm + WEIGHT_DECAY * w_norm)

    def stores(i):
        at = aligned(i * size, size)
        return [pltpu.make_async_copy(w.at[at], w_out.at[at], out_sem.at[0, i]), pltpu.make_async_copy(v.at[at], v_out.at[at], out_sem.at[1, i])]

    def update(i, carry):
        at = aligned(i * size, size)
        nv = MOMENTUM * v[at] + rate * (g[at] + WEIGHT_DECAY * w[at])
        v[at] = nv
        w[at] = w[at] - nv
        for copy in stores(i):
            copy.start()
        return carry

    def finish(i, carry):
        for copy in stores(i):
            copy.wait()
        return carry

    lax.fori_loop(0, parts, update, 0)
    lax.fori_loop(0, parts, finish, 0)


def conv_update(dep, lr, g, w, v):
    anywhere = pl.BlockSpec(memory_space=pl.ANY)
    dma = pltpu.SemaphoreType.DMA
    return pl.pallas_call(
        conv_update_kernel,
        in_specs=[pl.BlockSpec(memory_space=pltpu.VMEM), pl.BlockSpec(memory_space=pltpu.SMEM), anywhere, anywhere, anywhere],
        out_specs=[anywhere, anywhere],
        out_shape=[jax.ShapeDtypeStruct(w.shape, jnp.float32)] * 2,
        scratch_shapes=[pltpu.VMEM(w.shape, jnp.float32)] * 3 + [dma((3,)), dma((2, 8))],
        compiler_params=pltpu.CompilerParams(vmem_limit_bytes=VMEM_LIMIT),
        cost_estimate=pl.CostEstimate(flops=10 * w.size, bytes_accessed=20 * w.size, transcendentals=0),
        name="conv_update",
    )(dep, lr, g, w, v)


def gram_kernel(pos_count, scans, a, wc, gamma, beta, gcw_out, stats_out, asum_out, wb_out, gram, asum, parts):
    step = pl.program_id(0)
    c_mid = a.shape[-1]
    cols = wc.shape[1]

    @pl.when(step == 0)
    def _():
        gram[...] = jnp.zeros_like(gram)
        asum[...] = jnp.zeros_like(asum)

    @pl.when(step < scans)
    def _():
        x = a[...].reshape(-1, c_mid)
        gram[...] += lax.dot_general(x, x, (((0,), (0,)), ((), ())), preferred_element_type=jnp.float32)
        asum[...] += jnp.sum(x.astype(jnp.float32).reshape(-1, SUB, c_mid), axis=0)

    @pl.when(step == scans)
    def _():
        total = jnp.sum(asum[...], axis=0, keepdims=True)
        col = jnp.broadcast_to(total, (LANES, c_mid)).T
        asum_out[...] = col
        rest = gram[...] - tiled(col, c_mid // LANES) * (total / pos_count)
        for i in range(parts.shape[0]):
            part = rest.astype(jnp.bfloat16)
            parts[i] = part
            rest = rest - part.astype(jnp.float32)

    @pl.when(step >= scans)
    def _():
        wb = wc[...].astype(jnp.bfloat16)
        wb_out[...] = wb
        wr = wb.astype(jnp.float32)
        gcw = jnp.zeros((c_mid, cols), jnp.float32)
        for i in reversed(range(parts.shape[0])):
            gcw = gcw + jnp.dot(parts[i], wb, preferred_element_type=jnp.float32)
        gcw_out[...] = gcw
        var = jnp.maximum(jnp.sum(wr * gcw, axis=0, keepdims=True) / pos_count, 0.0)
        mean = jnp.sum(wr * tiled(asum_out[...], cols // LANES), axis=0, keepdims=True) / pos_count
        inv = lax.rsqrt(var + BN_EPS)
        scale = gamma[...] * inv
        stats_out[...] = stack_rows(mean, inv, scale, beta[...] - mean * scale)


def stack_rows(*rows):
    return jnp.concatenate(rows + (jnp.zeros_like(rows[0]),) * (SUB - len(rows)), axis=0)


def batch_stats(a3, w_conv, gamma, beta):
    spatial, per_dev, c_mid = a3.shape
    c_out = w_conv.shape[1]
    pos_count = spatial * per_dev
    scans = spatial // POS
    chunk = lambda rows: pl.BlockSpec((rows, CHUNK), lambda i: (0, jnp.maximum(i - scans, 0)))
    return pl.pallas_call(
        functools.partial(gram_kernel, pos_count, scans),
        grid=(scans + c_out // CHUNK,),
        in_specs=[pl.BlockSpec((POS, per_dev, c_mid), lambda i: (jnp.minimum(i, scans - 1), 0, 0)), chunk(c_mid), chunk(1), chunk(1)],
        out_specs=[chunk(c_mid), chunk(SUB), pl.BlockSpec((c_mid, LANES), lambda i: (0, 0)), chunk(c_mid)],
        out_shape=[
            jax.ShapeDtypeStruct((c_mid, c_out), jnp.float32),
            jax.ShapeDtypeStruct((SUB, c_out), jnp.float32),
            jax.ShapeDtypeStruct((c_mid, LANES), jnp.float32),
            jax.ShapeDtypeStruct((c_mid, c_out), jnp.bfloat16),
        ],
        scratch_shapes=[pltpu.VMEM((c_mid, c_mid), jnp.float32), pltpu.VMEM((SUB, c_mid), jnp.float32), pltpu.VMEM((3, c_mid, c_mid), jnp.bfloat16)],
        compiler_params=pltpu.CompilerParams(dimension_semantics=("arbitrary",), vmem_limit_bytes=VMEM_LIMIT),
        cost_estimate=pl.CostEstimate(flops=2 * pos_count * c_mid * c_mid, bytes_accessed=2 * pos_count * c_mid, transcendentals=0),
        name="batch_stats",
    )(a3, w_conv, gamma[None, :], beta[None, :])


def pool_kernel(spatial, a, s, wb, stats, p_out, n_out, mask_out):
    step = pl.program_id(0)
    wide = 2 * CHUNK

    @pl.when(step == 0)
    def _():
        p_out[...] = jnp.zeros_like(p_out)
        n_out[...] = jnp.zeros_like(n_out)

    def chunk(n, carry):
        cs = aligned(n * wide, wide)
        scale, shift = stats[2:3, cs], stats[3:4, cs]
        for j in range(POS):
            z = jnp.dot(a[j], wb[:, cs], preferred_element_type=jnp.float32)
            y = jnp.maximum(z * scale + shift + s[j, :, cs].astype(jnp.float32), 0.0)
            on = jnp.where(y.astype(jnp.bfloat16) > 0, jnp.bfloat16(1), jnp.bfloat16(0))
            mask_out[j, :, cs] = on
            p_out[:, cs] += y
            n_out[:, cs] += on
        return carry

    lax.fori_loop(0, p_out.shape[1] // wide, chunk, 0)

    @pl.when(step == pl.num_programs(0) - 1)
    def _():
        p_out[...] = p_out[...] * (1.0 / spatial)


def forward_pool(a3, s3, wb, stats):
    spatial, per_dev, c_mid = a3.shape
    c_out = wb.shape[1]
    fixed = lambda shape: pl.BlockSpec(shape, lambda i: (0,) * len(shape))
    part = lambda width: pl.BlockSpec((POS, per_dev, width), lambda i: (i, 0, 0))
    return pl.pallas_call(
        functools.partial(pool_kernel, spatial),
        grid=(spatial // POS,),
        in_specs=[part(c_mid), part(c_out), fixed(wb.shape), fixed(stats.shape)],
        out_specs=[fixed((per_dev, c_out)), fixed((per_dev, c_out)), part(c_out)],
        out_shape=[
            jax.ShapeDtypeStruct((per_dev, c_out), jnp.float32),
            jax.ShapeDtypeStruct((per_dev, c_out), jnp.bfloat16),
            jax.ShapeDtypeStruct((spatial, per_dev, c_out), jnp.bfloat16),
        ],
        compiler_params=pltpu.CompilerParams(dimension_semantics=("arbitrary",), vmem_limit_bytes=VMEM_LIMIT),
        cost_estimate=pl.CostEstimate(flops=2 * spatial * per_dev * c_mid * c_out, bytes_accessed=4 * spatial * per_dev * c_out, transcendentals=0),
        name="forward_pool",
    )(a3, s3, wb, stats)


def head_kernel(classes, global_rows, spatial, tiles, bsum, w_hbm, tail, bias, p, lab, wy, dpool_out, own_out, loss_out, wide_out, pt, wb, zb, acc, wsum, top, tot, ly, ring, sem):
    step = pl.program_id(0)
    rows, feats = p.shape
    width = ring.shape[1]
    now, prev = lax.rem(step, 2), lax.rem(step + 1, 2)
    left = classes - (tiles - 1) * width

    def fetch(i):
        slot = lax.rem(i, RING)
        return pltpu.make_async_copy(w_hbm.at[aligned(i * width, width)], ring.at[slot], sem.at[slot])

    def column(x):
        return jnp.broadcast_to(x, (LANES, rows)).T

    def logits(w):
        wb[now] = w
        b = jnp.broadcast_to(bias[...], (LANES, width)).T
        wide_out[...] = b
        half = width // 2
        for h in range(2):
            at = slice(h * half, (h + 1) * half)
            zb[now, at] = jnp.dot(w[at], pt[...], preferred_element_type=jnp.float32) + tiled(b[at], rows // LANES)

    @pl.when(step == 0)
    def _():
        for i in range(RING - 1):
            fetch(i).start()
        pt[...] = p[...].astype(jnp.bfloat16).T
        acc[...] = jnp.zeros_like(acc)
        wsum[...] = jnp.zeros_like(wsum)
        top[...] = jnp.full_like(top, -1e30)
        tot[...] = jnp.zeros_like(tot)
        ly[...] = jnp.zeros_like(ly)
        row = lax.broadcasted_iota(jnp.int32, (width, feats), 0)
        logits(jnp.where(row < left, tail[...], 0.0).astype(jnp.bfloat16))
        row = lax.broadcasted_iota(jnp.int32, (width, rows), 0)
        zb[now] = jnp.where(row < left, zb[now], -1e30)

    @pl.when(jnp.logical_and(step > 0, step < tiles))
    def _():
        fetch(step - 1).wait()

    @pl.when(jnp.logical_and(step > 0, step + RING - 2 < tiles - 1))
    def _():
        fetch(step + RING - 2).start()

    @pl.when(step > 0)
    def _():
        z = zb[prev]
        old = top[...]
        new = jnp.maximum(old, jnp.max(z, axis=0, keepdims=True))
        corr = jnp.exp(old - new)
        e = jnp.exp(z - new)
        top[...] = new
        tot[...] = tot[...] * corr + jnp.sum(e, axis=0, keepdims=True)
        base = jnp.where(step == 1, tiles - 1, step - 2) * width
        row = lax.broadcasted_iota(jnp.int32, (width, rows), 0) + base
        ly[...] += jnp.sum(jnp.where(lab[...] == row, z, 0.0), axis=0, keepdims=True)
        lead = jnp.concatenate([e.astype(jnp.bfloat16).T, jnp.ones((16, width), jnp.bfloat16)], axis=0)
        wide_corr = column(corr)
        logits(ring[lax.rem(step + RING - 1, RING)].astype(jnp.bfloat16))
        for n in range(feats // CHUNK):
            cs = slice(n * CHUNK, (n + 1) * CHUNK)
            part = jnp.dot(lead, wb[prev, :, cs], preferred_element_type=jnp.float32)
            acc[:, cs] = acc[:, cs] * tiled(wide_corr, CHUNK // LANES) + part[:rows]
            wsum[:, cs] += part[rows:rows + 8]

    @pl.when(step == tiles)
    def _():
        lse = top[...] + jnp.log(tot[...])
        ws = wsum[0:1, :]
        lsum = jnp.sum(pt[...].astype(jnp.float32) * tiled(jnp.broadcast_to(ws, (LANES, feats)).T, rows // LANES), axis=0, keepdims=True) + bsum[0]
        own_out[...] = jnp.concatenate([lse, lab[...].astype(jnp.float32)] + [jnp.zeros_like(lse)] * 6, axis=0)
        loss = lse - (1.0 - SMOOTHING) * ly[...] - SMOOTHING / classes * lsum
        loss_out[...] = jnp.full(loss_out.shape, jnp.sum(loss) * (1.0 / global_rows), jnp.float32)
        d = acc[...] / tiled(column(tot[...]), feats // LANES) - (1.0 - SMOOTHING) * wy[...] - SMOOTHING / classes * ws
        dpool_out[...] = d * (1.0 / (global_rows * spatial))


def head_pass(wt, bias, p, lab, wy, global_rows, spatial):
    classes, feats = wt.shape
    rows = p.shape[0]
    tiles = pl.cdiv(classes, WIDTH)
    fixed = lambda shape: pl.BlockSpec(shape, lambda i: (0,) * len(shape), pipeline_mode=pl.Buffered(1))
    kept = lambda shape: pl.BlockSpec(shape, lambda i: (0,) * len(shape))
    line = (1, rows)
    order = lambda i: jnp.where(i == 0, tiles - 1, jnp.minimum(i - 1, tiles - 2))
    return pl.pallas_call(
        functools.partial(head_kernel, classes, global_rows, spatial, tiles),
        grid=(tiles + 1,),
        in_specs=[
            pl.BlockSpec(memory_space=pltpu.SMEM),
            pl.BlockSpec(memory_space=pl.ANY),
            pl.BlockSpec((WIDTH, feats), lambda i: (tiles - 1, 0), pipeline_mode=pl.Buffered(1)),
            pl.BlockSpec((1, WIDTH), lambda i: (0, order(i))),
            fixed(p.shape), fixed(line), fixed(p.shape),
        ],
        out_specs=[kept(p.shape), kept((8, rows)), kept((8, LANES)), pl.BlockSpec((WIDTH, LANES), lambda i: (order(i), 0))],
        out_shape=[
            jax.ShapeDtypeStruct(p.shape, jnp.float32),
            jax.ShapeDtypeStruct((8, rows), jnp.float32),
            jax.ShapeDtypeStruct((8, LANES), jnp.float32),
            jax.ShapeDtypeStruct((tiles * WIDTH, LANES), jnp.float32),
        ],
        scratch_shapes=[
            pltpu.VMEM((feats, rows), jnp.bfloat16), pltpu.VMEM((2, WIDTH, feats), jnp.bfloat16), pltpu.VMEM((2, WIDTH, rows), jnp.float32),
            pltpu.VMEM(p.shape, jnp.float32), pltpu.VMEM((8, feats), jnp.float32),
        ] + [pltpu.VMEM(line, jnp.float32)] * 3 + [pltpu.VMEM((RING, WIDTH, feats), jnp.float32), pltpu.SemaphoreType.DMA((RING,))],
        compiler_params=pltpu.CompilerParams(dimension_semantics=("arbitrary",), vmem_limit_bytes=VMEM_LIMIT),
        cost_estimate=pl.CostEstimate(flops=4 * rows * feats * classes, bytes_accessed=4 * classes * feats, transcendentals=0),
        name="head_pass",
    )(jnp.sum(bias)[None], wt, wt, bias[None, :], p, lab[None, :], wy)


def conv_grad_kernel(pos_count, a, mask, dpool, n_on, stats, asum, gcw_hbm, wb_hbm, dconv_out, dgamma_out, dbeta_out, db, gcw, wb, sem):
    step = pl.program_id(0)
    c_mid = a.shape[-1]
    c_out = dpool.shape[1]
    late = [pltpu.make_async_copy(gcw_hbm, gcw, sem.at[0]), pltpu.make_async_copy(wb_hbm, wb, sem.at[1])]

    @pl.when(step == 0)
    def _():
        for copy in late:
            copy.start()
        db[...] = dpool[...].astype(jnp.bfloat16)
        dconv_out[...] = jnp.zeros_like(dconv_out)

    x = a[...].reshape(-1, c_mid)
    for n in range(c_out // CHUNK):
        cs = slice(n * CHUNK, (n + 1) * CHUNK)
        d = (mask[:, :, cs] * db[:, cs][None]).reshape(-1, CHUNK)
        dconv_out[:, cs] += lax.dot_general(x, d, (((0,), (0,)), ((), ())), preferred_element_type=jnp.float32)

    @pl.when(step == pl.num_programs(0) - 1)
    def _():
        for copy in late:
            copy.wait()

        def finish(n, carry):
            cs = aligned(n * CHUNK, CHUNK)
            mean, inv, scale = stats[0:1, cs], stats[1:2, cs], stats[2:3, cs]
            count = n_on[:, cs].astype(jnp.float32)
            dbeta_out[:, cs] = jnp.sum(dpool[:, cs] * count, axis=0, keepdims=True)
            dbeta = jnp.sum(db[:, cs].astype(jnp.float32) * count, axis=0, keepdims=True)
            m = dconv_out[:, cs]
            dgamma = inv * (jnp.sum(m * wb[:, cs].astype(jnp.float32), axis=0, keepdims=True) - mean * dbeta)
            dgamma_out[:, cs] = dgamma
            lead = tiled(asum[...], CHUNK // LANES)
            dconv_out[:, cs] = scale * (m - lead * (dbeta / pos_count) - gcw[:, cs] * (inv * dgamma / pos_count))
            return carry

        lax.fori_loop(0, c_out // CHUNK, finish, 0)


def conv_grad(a3, mask, dpool, n_on, stats, gcw, asum, wb):
    spatial, per_dev, c_mid = a3.shape
    c_out = wb.shape[1]
    pos_count = spatial * per_dev
    fixed = lambda a: pl.BlockSpec(a.shape, lambda i: (0, 0), pipeline_mode=pl.Buffered(1))
    part = lambda width: pl.BlockSpec((POS, per_dev, width), lambda i: (i, 0, 0))
    anywhere = pl.BlockSpec(memory_space=pl.ANY)
    kept = lambda rows: pl.BlockSpec((rows, c_out), lambda i: (0, 0))
    return pl.pallas_call(
        functools.partial(conv_grad_kernel, pos_count),
        grid=(spatial // POS,),
        in_specs=[part(c_mid), part(c_out), fixed(dpool), fixed(n_on), fixed(stats), fixed(asum), anywhere, anywhere],
        out_specs=[kept(c_mid), kept(1), kept(1)],
        out_shape=[jax.ShapeDtypeStruct((rows, c_out), jnp.float32) for rows in (c_mid, 1, 1)],
        scratch_shapes=[pltpu.VMEM(dpool.shape, jnp.bfloat16), pltpu.VMEM(gcw.shape, jnp.float32), pltpu.VMEM(wb.shape, jnp.bfloat16), pltpu.SemaphoreType.DMA((2,))],
        compiler_params=pltpu.CompilerParams(dimension_semantics=("arbitrary",), vmem_limit_bytes=VMEM_LIMIT),
        cost_estimate=pl.CostEstimate(flops=2 * pos_count * c_mid * c_out, bytes_accessed=2 * pos_count * c_out, transcendentals=0),
        name="conv_grad",
    )(a3, mask, dpool, n_on, stats, asum, gcw, wb)


def solution(mesh):
    groups = mesh.shape['dp']

    def local_step(act_in, shortcut, labels, w_conv, bn_gamma, bn_beta, w_fc, fc_bias, vel_conv, vel_gamma, vel_beta, vel_fc, vel_bias, learn_rate):
        per_dev = act_in.shape[0]
        global_rows = per_dev * groups
        spatial = act_in.shape[1] * act_in.shape[2]
        c_mid = act_in.shape[3]
        c_out = shortcut.shape[3]
        classes = w_fc.shape[1]
        dev = lax.axis_index('dp')
        wt, vt = w_fc.T, vel_fc.T
        a3 = act_in.reshape(per_dev, spatial, c_mid).transpose(1, 0, 2)
        s3 = shortcut.reshape(per_dev, spatial, c_out).transpose(1, 0, 2)
        gcw, stats, asum, wb = batch_stats(a3, w_conv, bn_gamma, bn_beta)
        pooled, n_on, mask = forward_pool(a3, s3, wb, stats)
        p_all = lax.all_gather(pooled, 'dp', tiled=True)
        wy = wt.at[labels].get(mode='promise_in_bounds')
        d_pool, own, loss_rows, bias_wide = head_pass(wt, fc_bias, pooled, labels, wy, global_rows, spatial)
        d_conv, d_gamma, d_beta = conv_grad(a3, mask, d_pool, n_on, stats, gcw, asum, wb)
        own, p_all, d_conv = lax.optimization_barrier((own, p_all, d_conv))
        lr = learn_rate[None]
        grads, p_bf, db, rows_in, rate = shared_grads(groups, wt, bias_wide, p_all, own, lr)
        n_tiles = pl.cdiv(classes, TILE)
        half = pl.cdiv(n_tiles, 2)
        db = jnp.sum(db[:half, :NORM * BLK], axis=-1) / global_rows
        d_bias = lax.dynamic_update_slice(jnp.zeros((half, 2, TILE), jnp.float32), db[:, None, :], (0, dev % 2, dev // 2 * NORM * BLK))
        vec = jnp.concatenate([d_bias.reshape(-1)[:classes], d_gamma[0], d_beta[0], loss_rows[0, :1]])
        g_conv, vec = lax.psum((d_conv, vec), 'dp')
        fc_new, fc_vel_new, dep = fused_update(rate, wt, vt, grads, bias_wide, p_bf, rows_in)
        conv_new, conv_vel_new = conv_update(dep, lr, g_conv, w_conv, vel_conv)
        g_bias, g_gamma, g_beta, loss_val = vec[:classes], vec[classes:classes + c_out], vec[classes + c_out:classes + 2 * c_out], vec[classes + 2 * c_out]
        gamma_vel_new = MOMENTUM * vel_gamma + learn_rate * g_gamma
        beta_vel_new = MOMENTUM * vel_beta + learn_rate * g_beta
        bias_vel_new = MOMENTUM * vel_bias + learn_rate * g_bias
        return (conv_new, bn_gamma - gamma_vel_new, bn_beta - beta_vel_new, fc_new.T, fc_bias - bias_vel_new, conv_vel_new, gamma_vel_new, beta_vel_new, fc_vel_new.T, bias_vel_new, loss_val)

    return jax.shard_map(local_step, mesh=mesh, in_specs=(P('dp'),) * 3 + (P(),) * 11, out_specs=(P(),) * 11, check_vma=False)
```

```python
import functools

import jax
import jax.numpy as jnp
from jax import lax
from jax.experimental import pallas as pl
from jax.experimental.pallas import tpu as pltpu
from jax.sharding import PartitionSpec as P

BN_EPS = 1e-5
SMOOTHING = 0.1
MOMENTUM = 0.9
TRUST_COEF = 0.001
WEIGHT_DECAY = 5e-5

TILE = 256
BLK = 32
SLOTS = TILE // BLK
HAVE = 3
NORM = 2
GROUP = 3
CHUNK = 512
POS = 7
WIDTH = 512
LANES = 128
SUB = 8
RING = 4
DEPTH = 3
VMEM_LIMIT = 66_000_000


def aligned(i, size):
    return pl.ds(pl.multiple_of(i, size), size)


def tiled(x, reps):
    return jnp.concatenate([x] * reps, axis=1)


def logit_grads(z, bias, lse, lab, base, classes):
    cols = z.shape[1]
    row = (lax.broadcasted_iota(jnp.int32, (BLK, cols), 0) + base).astype(jnp.float32)
    e = jnp.exp(z + tiled(bias, cols // LANES) - lse)
    low = SMOOTHING / classes
    return e - jnp.where(lab == row, low + (1.0 - SMOOTHING), low)


def grad_kernel(classes, groups, steps, *refs):
    nw = GROUP * HAVE
    ws, biases = refs[:nw], refs[nw:nw + GROUP]
    (p_all, own, lr, g_out, p_out, db_out, rows_out, rate_out, p, pbuf, lhs, dmat, gbuf, meta, sq, msg, msgs,
     p_sem, keep_sem, g_sem, gs_sem, gr_sem, meta_s, meta_r, msg_s, msg_r) = refs[nw + GROUP:]
    me = lax.axis_index('dp')
    q, c = me // 2, me % 2
    step = pl.program_id(0)
    rows_total, feats = p.shape
    per_dev = rows_total // groups

    def slot_of(i):
        return (2 * q + i) % SLOTS

    def base_of(group, k):
        return (2 * (GROUP * group + k // HAVE) + c) * TILE + slot_of(k % HAVE) * BLK

    def prepare(group):
        for k in range(nw):
            valid = lax.broadcasted_iota(jnp.int32, (BLK, feats), 0) < classes - base_of(group, k)
            w = jnp.where(valid, ws[k][...], 0.0)
            if k % HAVE < NORM:
                sq[1] += jnp.sum((w * w).reshape(BLK // 8, 8, feats), axis=0)
            lhs[group % 2, k * BLK:(k + 1) * BLK, :] = w.astype(jnp.bfloat16)

    def local(group):
        return pltpu.make_async_copy(gbuf.at[group % 2], g_out.at[c, pl.ds(group * GROUP, GROUP)], g_sem.at[group % 2])

    def remote(group):
        return pltpu.make_async_remote_copy(
            gbuf.at[group % 2], g_out.at[c, pl.ds(group * GROUP, GROUP)], gs_sem.at[group % 2], gr_sem.at[group],
            device_id=(me + 1 - 2 * c,), device_id_type=pl.DeviceIdType.MESH)

    def arrival(group):
        return pltpu.make_async_remote_copy(
            gbuf.at[group % 2], g_out.at[1 - c, pl.ds(group * GROUP, GROUP)], gs_sem.at[group % 2], gr_sem.at[group],
            device_id=(me + 1 - 2 * c,), device_id_type=pl.DeviceIdType.MESH)

    def spread(src, dst, send, recv):
        return [pltpu.make_async_remote_copy(
            src, dst.at[me], send.at[o], recv.at[o],
            device_id=((me + o) % groups,), device_id_type=pl.DeviceIdType.MESH) for o in range(1, groups)]

    keep = pltpu.make_async_copy(p, p_out, keep_sem)

    @pl.when(step == 0)
    def _():
        def fetch(i):
            return pltpu.make_async_copy(p_all.at[aligned(i * per_dev, per_dev)], pbuf.at[i], p_sem.at[i])

        for i in range(groups):
            fetch(i).start()
        barrier = pltpu.get_barrier_semaphore()
        for o in range(1, groups):
            pl.semaphore_signal(barrier, 1, device_id=((me + o) % groups,), device_id_type=pl.DeviceIdType.MESH)
        pl.semaphore_wait(barrier, groups - 1)
        for copy in spread(own, meta, meta_s, meta_r):
            copy.start()
        meta[me] = own[...]
        sq[...] = jnp.zeros_like(sq)
        prepare(0)

        def convert(i, carry):
            fetch(i).wait()
            p[aligned(i * per_dev, per_dev), :] = pbuf[i].astype(jnp.bfloat16)
            return carry

        lax.fori_loop(0, groups, convert, 0)
        keep.start()
        for copy in spread(own, meta, meta_s, meta_r):
            copy.wait()
        for d in range(groups):
            rows_out[:, d * per_dev:(d + 1) * per_dev] = meta[d]

    @pl.when(step > 1)
    def _():
        local(step - 2).start()
        remote(step - 2).start()

    @pl.when(step > 2)
    def _():
        local(step - 3).wait()
        remote(step - 3).wait_send()

    @pl.when(step > 0)
    def _():
        group = step - 1
        now = group % 2
        prepare(step)
        sums = [jnp.zeros((BLK, LANES), jnp.float32) for _ in range(nw)]
        for n in range(rows_total // CHUNK):
            cs = slice(n * CHUNK, (n + 1) * CHUNK)
            z = lax.dot_general(lhs[now], p[cs, :], (((1,), (1,)), ((), ())), preferred_element_type=jnp.float32)
            for k in range(nw):
                rs = slice(k * BLK, (k + 1) * BLK)
                bias = biases[k // HAVE][aligned(slot_of(k % HAVE) * BLK, BLK), :]
                d = logit_grads(z[rs], bias, rows_out[0:1, cs], rows_out[1:2, cs], base_of(group, k), classes)
                valid = lax.broadcasted_iota(jnp.int32, (BLK, CHUNK), 0) < classes - base_of(group, k)
                d = jnp.where(valid, d, 0.0)
                for m in range(CHUNK // LANES):
                    sums[k] = sums[k] + d[:, m * LANES:(m + 1) * LANES]
                dmat[rs, cs] = d.astype(jnp.bfloat16)
        lane = lax.broadcasted_iota(jnp.int32, (1, TILE), 1)
        db_out[...] = jnp.zeros_like(db_out)
        for t in range(GROUP):
            line = jnp.zeros((1, TILE), jnp.float32)
            for i in range(NORM):
                row = jnp.sum(sums[t * HAVE + i].T, axis=0, keepdims=True)
                line = jnp.where(lane // BLK == slot_of(i), tiled(row, SLOTS), line)
            db_out[0, pl.ds(2 * t + c, 1), :] = line * (1.0 / rows_total)
        for n in range(feats // CHUNK):
            cs = slice(n * CHUNK, (n + 1) * CHUNK)
            g = jnp.dot(dmat[...], p[:, cs], preferred_element_type=jnp.float32) * (1.0 / rows_total)
            for k in range(nw):
                gk = g[k * BLK:(k + 1) * BLK]
                gbuf[now, k // HAVE, (k % HAVE) * BLK:(k % HAVE + 1) * BLK, cs] = gk
                if k % HAVE < NORM:
                    sq[0, :, cs] += jnp.sum((gk * gk).reshape(BLK // 8, 8, CHUNK), axis=0)

    @pl.when(step == steps)
    def _():
        for i in range(2):
            parts = sq[i]
            total = parts[:, 0:LANES]
            for m in range(1, feats // LANES):
                total = total + parts[:, m * LANES:(m + 1) * LANES]
            msg[i] = total
        local(steps - 1).start()
        remote(steps - 1).start()
        keep.wait()
        local(steps - 2).wait()
        remote(steps - 2).wait_send()
        for copy in spread(msg, msgs, msg_s, msg_r):
            copy.start()
        msgs[me] = msg[...]
        local(steps - 1).wait()
        remote(steps - 1).wait_send()
        for group in range(steps):
            arrival(group).wait_recv()
        for copy in spread(msg, msgs, msg_s, msg_r):
            copy.wait()
        both = jnp.sum(msgs[...], axis=0)
        g_norm = jnp.sqrt(jnp.sum(both[0]))
        w_norm = jnp.sqrt(jnp.sum(both[1]))
        rate_out[...] = jnp.full(rate_out.shape, lr[0] * TRUST_COEF * w_norm / (g_norm + WEIGHT_DECAY * w_norm), jnp.float32)


def shared_grads(groups, wt, bias, p_all, own, lr):
    classes, feats = wt.shape
    rows_total = p_all.shape[0]
    n_tiles = pl.cdiv(classes, TILE)
    steps = pl.cdiv(pl.cdiv(n_tiles, 2), GROUP)
    last = pl.cdiv(classes, BLK) - 1

    def w_map(t, i):
        def index(s):
            me = lax.axis_index('dp')
            tile = 2 * (GROUP * jnp.minimum(s, steps - 1) + t) + me % 2
            return jnp.minimum(tile * SLOTS + (2 * (me // 2) + i) % SLOTS, last), 0
        return index

    def b_map(t):
        return lambda s: (jnp.minimum(2 * (GROUP * jnp.maximum(s - 1, 0) + t) + lax.axis_index('dp') % 2, n_tiles - 1), 0)

    rows = GROUP * HAVE * BLK
    anywhere = pl.BlockSpec(memory_space=pl.ANY)
    dma = pltpu.SemaphoreType.DMA
    return pl.pallas_call(
        functools.partial(grad_kernel, classes, groups, steps),
        grid=(steps + 1,),
        in_specs=[pl.BlockSpec((BLK, feats), w_map(t, i)) for t in range(GROUP) for i in range(HAVE)]
        + [pl.BlockSpec((TILE, LANES), b_map(t)) for t in range(GROUP)]
        + [anywhere, pl.BlockSpec(own.shape, lambda s: (0, 0)), pl.BlockSpec(memory_space=pltpu.SMEM)],
        out_specs=[
            anywhere, anywhere,
            pl.BlockSpec((1, 2 * GROUP, TILE), lambda s: (jnp.maximum(s - 1, 0), 0, 0)),
            pl.BlockSpec((8, rows_total), lambda s: (0, 0)),
            pl.BlockSpec((8, LANES), lambda s: (0, 0)),
        ],
        out_shape=[
            jax.ShapeDtypeStruct((2, steps * GROUP, HAVE * BLK, feats), jnp.float32),
            jax.ShapeDtypeStruct((rows_total, feats), jnp.bfloat16),
            jax.ShapeDtypeStruct((steps, 2 * GROUP, TILE), jnp.float32),
            jax.ShapeDtypeStruct((8, rows_total), jnp.float32),
            jax.ShapeDtypeStruct((8, LANES), jnp.float32),
        ],
        scratch_shapes=[
            pltpu.VMEM((rows_total, feats), jnp.bfloat16),
            pltpu.VMEM((groups, rows_total // groups, feats), jnp.float32),
            pltpu.VMEM((2, rows, feats), jnp.bfloat16), pltpu.VMEM((rows, rows_total), jnp.bfloat16),
            pltpu.VMEM((2, GROUP, HAVE * BLK, feats), jnp.float32),
            pltpu.VMEM((groups,) + own.shape, jnp.float32),
            pltpu.VMEM((2, 8, feats), jnp.float32), pltpu.VMEM((2, 8, LANES), jnp.float32), pltpu.VMEM((groups, 2, 8, LANES), jnp.float32),
            dma((groups,)), dma, dma((2,)), dma((2,)), dma((steps,)),
            dma((groups,)), dma((groups,)), dma((groups,)), dma((groups,)),
        ],
        compiler_params=pltpu.CompilerParams(dimension_semantics=("arbitrary",), vmem_limit_bytes=VMEM_LIMIT, collective_id=0, has_side_effects=True),
        cost_estimate=pl.CostEstimate(flops=4 * steps * rows * feats * rows_total, bytes_accessed=8 * steps * rows * feats, transcendentals=0),
        name="shared_grads",
    )(*([wt] * (GROUP * HAVE)), *([bias] * GROUP), p_all, own, lr)


def update_kernel(classes, steps, rate, w_hbm, v_hbm, w_end, v_end, even, odd, bias, p, rows_in, w_out, v_out, done, wbuf, vbuf, lhs, dmat, w_sem, v_sem):
    q = lax.axis_index('dp') // 2
    step = pl.program_id(0)
    a = tiled(rate[0:1, :], CHUNK // LANES)
    cols, feats = p.shape
    tall = 2 * TILE
    whole = (classes - (steps - 1) * tall) // SUB * SUB
    done[...] = jnp.zeros_like(done)

    def fetch(i, act, hbm, buf, sem):
        slot = lax.rem(i, DEPTH)

        def go(size):
            act(pltpu.make_async_copy(hbm.at[pl.ds(pl.multiple_of(i * tall, tall), size)], buf.at[slot, pl.ds(0, size)], sem.at[slot]))

        @pl.when(i < steps - 1)
        def _():
            go(tall)

        @pl.when(i == steps - 1)
        def _():
            go(whole)

    start = lambda copy: copy.start()
    wait = lambda copy: copy.wait()

    def arrived(i, hbm, buf, sem, end):
        fetch(i, wait, hbm, buf, sem)

        @pl.when(i == steps - 1)
        def _():
            buf[lax.rem(i, DEPTH), whole:whole + SUB, :] = end[...]

    slot = lax.rem(step, DEPTH)

    def apply(rs, cs, g):
        w = wbuf[slot, rs, cs]
        nv = MOMENTUM * vbuf[slot, rs, cs] + a * (g + WEIGHT_DECAY * w)
        v_out[rs, cs] = nv
        w_out[rs, cs] = w - nv

    bases = []
    for t in range(2):
        for i in range(HAVE, SLOTS):
            bases.append(t * TILE + (2 * q + i) % SLOTS * BLK)

    @pl.when(step == 0)
    def _():
        for i in range(2):
            fetch(i, start, w_hbm, wbuf, w_sem)
            fetch(i, start, v_hbm, vbuf, v_sem)

    arrived(step, w_hbm, wbuf, w_sem, w_end)
    arrived(step, v_hbm, vbuf, v_sem, v_end)
    fetch(step + 2, start, w_hbm, wbuf, w_sem)
    fetch(step + 2, start, v_hbm, vbuf, v_sem)
    for k, base in enumerate(bases):
        lhs[k * BLK:(k + 1) * BLK, :] = wbuf[slot, aligned(base, BLK), :].astype(jnp.bfloat16)
    for n in range(cols // CHUNK):
        cs = slice(n * CHUNK, (n + 1) * CHUNK)
        z = lax.dot_general(lhs[...], p[cs, :], (((1,), (1,)), ((), ())), preferred_element_type=jnp.float32)
        for t, src in enumerate((even, odd)):
            for i in range(HAVE):
                apply(aligned(t * TILE + (2 * q + i) % SLOTS * BLK, BLK), cs, src[0, 0, i * BLK:(i + 1) * BLK, cs])
        for k, base in enumerate(bases):
            rs = slice(k * BLK, (k + 1) * BLK)
            d = logit_grads(z[rs], bias[aligned(base, BLK), :], rows_in[0:1, cs], rows_in[1:2, cs], step * tall + base, classes)
            dmat[rs, cs] = d.astype(jnp.bfloat16)

    for n in range(feats // CHUNK):
        cs = slice(n * CHUNK, (n + 1) * CHUNK)
        g = jnp.dot(dmat[...], p[:, cs], preferred_element_type=jnp.float32) * (1.0 / cols)
        for k, base in enumerate(bases):
            apply(aligned(base, BLK), cs, g[k * BLK:(k + 1) * BLK])


def fused_update(rate, wt, vt, grads, bias, p, rows_in):
    classes, feats = wt.shape
    tall = 2 * TILE
    steps = pl.cdiv(classes, tall)
    whole = lambda a: pl.BlockSpec(a.shape, lambda s: (0, 0), pipeline_mode=pl.Buffered(1))
    anywhere = pl.BlockSpec(memory_space=pl.ANY)
    end = pl.BlockSpec((SUB, feats), lambda s: (classes // SUB, 0), pipeline_mode=pl.Buffered(1))
    tile = pl.BlockSpec((tall, feats), lambda s: (s, 0))
    part = lambda par: pl.BlockSpec((1, 1, HAVE * BLK, feats), lambda s: (par, s, 0, 0))
    rows = 2 * (SLOTS - HAVE) * BLK
    dma = pltpu.SemaphoreType.DMA
    return pl.pallas_call(
        functools.partial(update_kernel, classes, steps),
        grid=(steps,),
        in_specs=[whole(rate), anywhere, anywhere, end, end, part(0), part(1), pl.BlockSpec((tall, LANES), lambda s: (s, 0)), whole(p), whole(rows_in)],
        out_specs=[tile, tile, pl.BlockSpec((SUB, LANES), lambda s: (0, 0))],
        scratch_shapes=[
            pltpu.VMEM((DEPTH, tall, feats), jnp.float32), pltpu.VMEM((DEPTH, tall, feats), jnp.float32),
            pltpu.VMEM((rows, feats), jnp.bfloat16), pltpu.VMEM((rows, p.shape[0]), jnp.bfloat16), dma((DEPTH,)), dma((DEPTH,)),
        ],
        out_shape=[jax.ShapeDtypeStruct(wt.shape, jnp.float32)] * 2 + [jax.ShapeDtypeStruct((SUB, LANES), jnp.float32)],
        compiler_params=pltpu.CompilerParams(dimension_semantics=("arbitrary",), vmem_limit_bytes=VMEM_LIMIT),
        cost_estimate=pl.CostEstimate(flops=4 * steps * rows * feats * p.shape[0], bytes_accessed=16 * classes * feats, transcendentals=0),
        name="fused_update",
    )(rate, wt, vt, wt, vt, grads, grads, bias, p, rows_in)


def conv_update_kernel(dep, lr, g_hbm, w_hbm, v_hbm, w_out, v_out, g, w, v, sem, out_sem):
    loads = [pltpu.make_async_copy(x, y, sem.at[i]) for i, (x, y) in enumerate(((g_hbm, g), (w_hbm, w), (v_hbm, v)))]
    for copy in loads:
        copy.start()
    parts = out_sem.shape[1]
    size = g.shape[0] // parts

    def square_sum(ref):
        def add(i, acc):
            x = ref[aligned(i * size, size)]
            return acc + jnp.sum((x * x).reshape(size // SUB, SUB, x.shape[1]), axis=0)
        return jnp.sum(lax.fori_loop(0, parts, add, jnp.zeros((SUB, ref.shape[1]), jnp.float32)))

    loads[0].wait()
    g_norm = jnp.sqrt(square_sum(g))
    loads[1].wait()
    w_norm = jnp.sqrt(square_sum(w))
    loads[2].wait()
    rate = lr[0] * TRUST_COEF * w_norm / (g_norm + WEIGHT_DECAY * w_norm)

    def stores(i):
        at = aligned(i * size, size)
        return [pltpu.make_async_copy(w.at[at], w_out.at[at], out_sem.at[0, i]), pltpu.make_async_copy(v.at[at], v_out.at[at], out_sem.at[1, i])]

    def update(i, carry):
        at = aligned(i * size, size)
        nv = MOMENTUM * v[at] + rate * (g[at] + WEIGHT_DECAY * w[at])
        v[at] = nv
        w[at] = w[at] - nv
        for copy in stores(i):
            copy.start()
        return carry

    def finish(i, carry):
        for copy in stores(i):
            copy.wait()
        return carry

    lax.fori_loop(0, parts, update, 0)
    lax.fori_loop(0, parts, finish, 0)


def conv_update(dep, lr, g, w, v):
    anywhere = pl.BlockSpec(memory_space=pl.ANY)
    dma = pltpu.SemaphoreType.DMA
    return pl.pallas_call(
        conv_update_kernel,
        in_specs=[pl.BlockSpec(memory_space=pltpu.VMEM), pl.BlockSpec(memory_space=pltpu.SMEM), anywhere, anywhere, anywhere],
        out_specs=[anywhere, anywhere],
        out_shape=[jax.ShapeDtypeStruct(w.shape, jnp.float32)] * 2,
        scratch_shapes=[pltpu.VMEM(w.shape, jnp.float32)] * 3 + [dma((3,)), dma((2, 8))],
        compiler_params=pltpu.CompilerParams(vmem_limit_bytes=VMEM_LIMIT),
        cost_estimate=pl.CostEstimate(flops=10 * w.size, bytes_accessed=20 * w.size, transcendentals=0),
        name="conv_update",
    )(dep, lr, g, w, v)


def front_kernel(spatial, scans, chunks, a_hbm, s, wc, gamma, beta, gcw_out, stats_out, asum_out, wb_out, p_out, y_out, a, gram, asum, parts, wb, stats, sem):
    step = pl.program_id(0)
    c_mid = a.shape[-1]
    cols = wc.shape[1]
    pos_count = spatial * a.shape[1]
    wide = 2 * CHUNK

    def fetch(i):
        at = pl.ds(i * POS, POS)
        return pltpu.make_async_copy(a_hbm.at[at], a.at[at], sem.at[i])

    @pl.when(step == 0)
    def _():
        for i in range(scans):
            fetch(i).start()
        gram[...] = jnp.zeros_like(gram)
        asum[...] = jnp.zeros_like(asum)
        p_out[...] = jnp.zeros_like(p_out)

    @pl.when(step < scans)
    def _():
        fetch(step).wait()
        x = a[pl.ds(step * POS, POS)].reshape(-1, c_mid)
        gram[...] += lax.dot_general(x, x, (((0,), (0,)), ((), ())), preferred_element_type=jnp.float32)
        asum[...] += jnp.sum(x.astype(jnp.float32).reshape(-1, SUB, c_mid), axis=0)

    @pl.when(step == scans)
    def _():
        total = jnp.sum(asum[...], axis=0, keepdims=True)
        col = jnp.broadcast_to(total, (LANES, c_mid)).T
        asum_out[...] = col
        rest = gram[...] - tiled(col, c_mid // LANES) * (total / pos_count)
        for i in range(parts.shape[0]):
            part = rest.astype(jnp.bfloat16)
            parts[i] = part
            rest = rest - part.astype(jnp.float32)

    @pl.when(jnp.logical_and(step >= scans, step < scans + chunks))
    def _():
        at = aligned((step - scans) * cols, cols)
        w = wc[...].astype(jnp.bfloat16)
        wb_out[...] = w
        wb[:, at] = w
        wr = w.astype(jnp.float32)
        gcw = jnp.zeros((c_mid, cols), jnp.float32)
        for i in reversed(range(parts.shape[0])):
            gcw = gcw + jnp.dot(parts[i], w, preferred_element_type=jnp.float32)
        gcw_out[...] = gcw
        var = jnp.maximum(jnp.sum(wr * gcw, axis=0, keepdims=True) / pos_count, 0.0)
        mean = jnp.sum(wr * tiled(asum_out[...], cols // LANES), axis=0, keepdims=True) / pos_count
        inv = lax.rsqrt(var + BN_EPS)
        scale = gamma[...] * inv
        rows = (mean, inv, scale, beta[...] - mean * scale)
        rows = jnp.concatenate(rows + (jnp.zeros_like(inv),) * (SUB - len(rows)), axis=0)
        stats_out[...] = rows
        stats[:, at] = rows

    @pl.when(step >= scans + chunks)
    def _():
        first = (step - scans - chunks) * POS

        def chunk(n, carry):
            cs = aligned(n * wide, wide)
            scale, shift = stats[2:3, cs], stats[3:4, cs]
            for j in range(POS):
                z = jnp.dot(a[first + j], wb[:, cs], preferred_element_type=jnp.float32)
                y = jnp.maximum(z * scale + shift + s[j, :, cs].astype(jnp.float32), 0.0)
                y_out[j, :, cs] = y.astype(jnp.bfloat16)
                p_out[:, cs] += y
            return carry

        lax.fori_loop(0, p_out.shape[1] // wide, chunk, 0)

    @pl.when(step == pl.num_programs(0) - 1)
    def _():
        p_out[...] = p_out[...] * (1.0 / spatial)


def front(a3, s3, w_conv, gamma, beta):
    spatial, per_dev, c_mid = a3.shape
    c_out = w_conv.shape[1]
    scans, chunks = spatial // POS, c_out // CHUNK
    fixed = lambda shape: pl.BlockSpec(shape, lambda i: (0, 0))
    chunk = lambda rows: pl.BlockSpec((rows, CHUNK), lambda i: (0, jnp.clip(i - scans, 0, chunks - 1)))
    part = pl.BlockSpec((POS, per_dev, c_out), lambda i: (jnp.maximum(i - scans - chunks, 0), 0, 0))
    return pl.pallas_call(
        functools.partial(front_kernel, spatial, scans, chunks),
        grid=(2 * scans + chunks,),
        in_specs=[pl.BlockSpec(memory_space=pl.ANY), part, chunk(c_mid), chunk(1), chunk(1)],
        out_specs=[chunk(c_mid), chunk(SUB), fixed((c_mid, LANES)), chunk(c_mid), fixed((per_dev, c_out)), part],
        out_shape=[
            jax.ShapeDtypeStruct((c_mid, c_out), jnp.float32),
            jax.ShapeDtypeStruct((SUB, c_out), jnp.float32),
            jax.ShapeDtypeStruct((c_mid, LANES), jnp.float32),
            jax.ShapeDtypeStruct((c_mid, c_out), jnp.bfloat16),
            jax.ShapeDtypeStruct((per_dev, c_out), jnp.float32),
            jax.ShapeDtypeStruct((spatial, per_dev, c_out), jnp.bfloat16),
        ],
        scratch_shapes=[
            pltpu.VMEM(a3.shape, jnp.bfloat16), pltpu.VMEM((c_mid, c_mid), jnp.float32), pltpu.VMEM((SUB, c_mid), jnp.float32),
            pltpu.VMEM((3, c_mid, c_mid), jnp.bfloat16), pltpu.VMEM((c_mid, c_out), jnp.bfloat16), pltpu.VMEM((SUB, c_out), jnp.float32),
            pltpu.SemaphoreType.DMA((scans,)),
        ],
        compiler_params=pltpu.CompilerParams(dimension_semantics=("arbitrary",), vmem_limit_bytes=VMEM_LIMIT),
        cost_estimate=pl.CostEstimate(flops=2 * spatial * per_dev * c_mid * (c_mid + c_out), bytes_accessed=4 * spatial * per_dev * c_out, transcendentals=0),
        name="front",
    )(a3, s3, w_conv, gamma[None, :], beta[None, :])


def head_kernel(classes, global_rows, spatial, tiles, bsum, lab_s, w_hbm, tail, bias, p, lab, dpool_out, own_out, loss_out, wide_out, pt, wb, zb, acc, wsum, top, tot, ly, ring, wy, sem, row_sem):
    step = pl.program_id(0)
    rows, feats = p.shape
    width = ring.shape[1]
    now, prev = lax.rem(step, 2), lax.rem(step + 1, 2)
    left = classes - (tiles - 1) * width

    def fetch(i):
        slot = lax.rem(i, RING)
        return pltpu.make_async_copy(w_hbm.at[aligned(i * width, width)], ring.at[slot], sem.at[slot])

    def pick(i):
        return pltpu.make_async_copy(w_hbm.at[pl.ds(lab_s[i], 1)], wy.at[pl.ds(i, 1)], row_sem)

    def column(x):
        return jnp.broadcast_to(x, (LANES, rows)).T

    def logits(w):
        wb[now] = w
        b = jnp.broadcast_to(bias[...], (LANES, width)).T
        wide_out[...] = b
        half = width // 2
        for h in range(2):
            at = slice(h * half, (h + 1) * half)
            zb[now, at] = jnp.dot(w[at], pt[...], preferred_element_type=jnp.float32) + tiled(b[at], rows // LANES)

    @pl.when(step == 0)
    def _():
        for i in range(RING - 1):
            fetch(i).start()

        def begin(i, carry):
            pick(i).start()
            return carry

        lax.fori_loop(0, rows, begin, 0)
        pt[...] = p[...].astype(jnp.bfloat16).T
        acc[...] = jnp.zeros_like(acc)
        wsum[...] = jnp.zeros_like(wsum)
        top[...] = jnp.full_like(top, -1e30)
        tot[...] = jnp.zeros_like(tot)
        ly[...] = jnp.zeros_like(ly)
        row = lax.broadcasted_iota(jnp.int32, (width, feats), 0)
        logits(jnp.where(row < left, tail[...], 0.0).astype(jnp.bfloat16))
        row = lax.broadcasted_iota(jnp.int32, (width, rows), 0)
        zb[now] = jnp.where(row < left, zb[now], -1e30)

    @pl.when(jnp.logical_and(step > 0, step < tiles))
    def _():
        fetch(step - 1).wait()

    @pl.when(jnp.logical_and(step > 0, step + RING - 2 < tiles - 1))
    def _():
        fetch(step + RING - 2).start()

    @pl.when(step > 0)
    def _():
        z = zb[prev]
        old = top[...]
        new = jnp.maximum(old, jnp.max(z, axis=0, keepdims=True))
        corr = jnp.exp(old - new)
        e = jnp.exp(z - new)
        top[...] = new
        tot[...] = tot[...] * corr + jnp.sum(e, axis=0, keepdims=True)
        base = jnp.where(step == 1, tiles - 1, step - 2) * width
        row = lax.broadcasted_iota(jnp.int32, (width, rows), 0) + base
        ly[...] += jnp.sum(jnp.where(lab[...] == row, z, 0.0), axis=0, keepdims=True)
        lead = jnp.concatenate([e.astype(jnp.bfloat16).T, jnp.ones((16, width), jnp.bfloat16)], axis=0)
        wide_corr = column(corr)
        logits(ring[lax.rem(step + RING - 1, RING)].astype(jnp.bfloat16))
        for n in range(feats // CHUNK):
            cs = slice(n * CHUNK, (n + 1) * CHUNK)
            part = jnp.dot(lead, wb[prev, :, cs], preferred_element_type=jnp.float32)
            acc[:, cs] = acc[:, cs] * tiled(wide_corr, CHUNK // LANES) + part[:rows]
            wsum[:, cs] += part[rows:rows + 8]

    @pl.when(step == tiles)
    def _():
        pltpu.make_async_copy(w_hbm.at[pl.ds(0, rows)], wy, row_sem).wait()
        lse = top[...] + jnp.log(tot[...])
        ws = wsum[0:1, :]
        lsum = jnp.sum(pt[...].astype(jnp.float32) * tiled(jnp.broadcast_to(ws, (LANES, feats)).T, rows // LANES), axis=0, keepdims=True) + bsum[0]
        own_out[...] = jnp.concatenate([lse, lab[...].astype(jnp.float32)] + [jnp.zeros_like(lse)] * 6, axis=0)
        loss = lse - (1.0 - SMOOTHING) * ly[...] - SMOOTHING / classes * lsum
        loss_out[0] = jnp.sum(loss) * (1.0 / global_rows)
        d = acc[...] / tiled(column(tot[...]), feats // LANES) - (1.0 - SMOOTHING) * wy[...] - SMOOTHING / classes * ws
        dpool_out[...] = d * (1.0 / (global_rows * spatial))


def head_pass(wt, bias, p, lab, global_rows, spatial):
    classes, feats = wt.shape
    rows = p.shape[0]
    tiles = pl.cdiv(classes, WIDTH)
    fixed = lambda shape: pl.BlockSpec(shape, lambda i: (0,) * len(shape), pipeline_mode=pl.Buffered(1))
    kept = lambda shape: pl.BlockSpec(shape, lambda i: (0,) * len(shape))
    line = (1, rows)
    order = lambda i: jnp.where(i == 0, tiles - 1, jnp.minimum(i - 1, tiles - 2))
    return pl.pallas_call(
        functools.partial(head_kernel, classes, global_rows, spatial, tiles),
        grid=(tiles + 1,),
        in_specs=[
            pl.BlockSpec(memory_space=pltpu.SMEM),
            pl.BlockSpec(memory_space=pltpu.SMEM),
            pl.BlockSpec(memory_space=pl.ANY),
            pl.BlockSpec((WIDTH, feats), lambda i: (tiles - 1, 0), pipeline_mode=pl.Buffered(1)),
            pl.BlockSpec((1, WIDTH), lambda i: (0, order(i))),
            fixed(p.shape), fixed(line),
        ],
        out_specs=[kept(p.shape), kept((8, rows)), pl.BlockSpec(memory_space=pltpu.SMEM), pl.BlockSpec((WIDTH, LANES), lambda i: (order(i), 0))],
        out_shape=[
            jax.ShapeDtypeStruct(p.shape, jnp.float32),
            jax.ShapeDtypeStruct((8, rows), jnp.float32),
            jax.ShapeDtypeStruct((1,), jnp.float32),
            jax.ShapeDtypeStruct((tiles * WIDTH, LANES), jnp.float32),
        ],
        scratch_shapes=[
            pltpu.VMEM((feats, rows), jnp.bfloat16), pltpu.VMEM((2, WIDTH, feats), jnp.bfloat16), pltpu.VMEM((2, WIDTH, rows), jnp.float32),
            pltpu.VMEM(p.shape, jnp.float32), pltpu.VMEM((8, feats), jnp.float32),
        ] + [pltpu.VMEM(line, jnp.float32)] * 3 + [pltpu.VMEM((RING, WIDTH, feats), jnp.float32), pltpu.VMEM(p.shape, jnp.float32), pltpu.SemaphoreType.DMA((RING,)), pltpu.SemaphoreType.DMA],
        compiler_params=pltpu.CompilerParams(dimension_semantics=("arbitrary",), vmem_limit_bytes=VMEM_LIMIT),
        cost_estimate=pl.CostEstimate(flops=4 * rows * feats * classes, bytes_accessed=4 * classes * feats, transcendentals=0),
        name="head_pass",
    )(jnp.sum(bias)[None], lab, wt, wt, bias[None, :], p, lab[None, :])


def conv_grad_kernel(pos_count, a, y, dpool, stats, asum, gcw_hbm, wb_hbm, dconv_out, dgamma_out, dbeta_out, db, n_on, gcw, wb, sem):
    step = pl.program_id(0)
    c_mid = a.shape[-1]
    c_out = dpool.shape[1]
    late = [pltpu.make_async_copy(gcw_hbm, gcw, sem.at[0]), pltpu.make_async_copy(wb_hbm, wb, sem.at[1])]

    @pl.when(step == 0)
    def _():
        for copy in late:
            copy.start()
        db[...] = dpool[...].astype(jnp.bfloat16)
        dconv_out[...] = jnp.zeros_like(dconv_out)
        n_on[...] = jnp.zeros_like(n_on)

    x = a[...].reshape(-1, c_mid)
    for n in range(c_out // CHUNK):
        cs = slice(n * CHUNK, (n + 1) * CHUNK)
        on = y[:, :, cs] > 0
        ones = jnp.where(on, jnp.bfloat16(1), jnp.bfloat16(0))
        count = ones[0]
        for j in range(1, POS):
            count = count + ones[j]
        n_on[:, cs] += count
        d = (ones * db[:, cs][None]).reshape(-1, CHUNK)
        dconv_out[:, cs] += lax.dot_general(x, d, (((0,), (0,)), ((), ())), preferred_element_type=jnp.float32)

    @pl.when(step == pl.num_programs(0) - 1)
    def _():
        for copy in late:
            copy.wait()

        def finish(n, carry):
            cs = aligned(n * CHUNK, CHUNK)
            mean, inv, scale = stats[0:1, cs], stats[1:2, cs], stats[2:3, cs]
            count = n_on[:, cs].astype(jnp.float32)
            dbeta_out[:, cs] = jnp.sum(dpool[:, cs] * count, axis=0, keepdims=True)
            dbeta = jnp.sum(db[:, cs].astype(jnp.float32) * count, axis=0, keepdims=True)
            m = dconv_out[:, cs]
            dgamma = inv * (jnp.sum(m * wb[:, cs].astype(jnp.float32), axis=0, keepdims=True) - mean * dbeta)
            dgamma_out[:, cs] = dgamma
            lead = tiled(asum[...], CHUNK // LANES)
            dconv_out[:, cs] = scale * (m - lead * (dbeta / pos_count) - gcw[:, cs] * (inv * dgamma / pos_count))
            return carry

        lax.fori_loop(0, c_out // CHUNK, finish, 0)


def conv_grad(a3, y, dpool, stats, gcw, asum, wb):
    spatial, per_dev, c_mid = a3.shape
    c_out = wb.shape[1]
    pos_count = spatial * per_dev
    fixed = lambda a: pl.BlockSpec(a.shape, lambda i: (0, 0), pipeline_mode=pl.Buffered(1))
    part = lambda width: pl.BlockSpec((POS, per_dev, width), lambda i: (i, 0, 0))
    anywhere = pl.BlockSpec(memory_space=pl.ANY)
    kept = lambda rows: pl.BlockSpec((rows, c_out), lambda i: (0, 0))
    return pl.pallas_call(
        functools.partial(conv_grad_kernel, pos_count),
        grid=(spatial // POS,),
        in_specs=[part(c_mid), part(c_out), fixed(dpool), fixed(stats), fixed(asum), anywhere, anywhere],
        out_specs=[kept(c_mid), kept(1), kept(1)],
        out_shape=[jax.ShapeDtypeStruct((rows, c_out), jnp.float32) for rows in (c_mid, 1, 1)],
        scratch_shapes=[pltpu.VMEM(dpool.shape, jnp.bfloat16), pltpu.VMEM(dpool.shape, jnp.bfloat16), pltpu.VMEM(gcw.shape, jnp.float32), pltpu.VMEM(wb.shape, jnp.bfloat16), pltpu.SemaphoreType.DMA((2,))],
        compiler_params=pltpu.CompilerParams(dimension_semantics=("arbitrary",), vmem_limit_bytes=VMEM_LIMIT),
        cost_estimate=pl.CostEstimate(flops=2 * pos_count * c_mid * c_out, bytes_accessed=2 * pos_count * c_out, transcendentals=0),
        name="conv_grad",
    )(a3, y, dpool, stats, asum, gcw, wb)


def solution(mesh):
    groups = mesh.shape['dp']

    def local_step(act_in, shortcut, labels, w_conv, bn_gamma, bn_beta, w_fc, fc_bias, vel_conv, vel_gamma, vel_beta, vel_fc, vel_bias, learn_rate):
        per_dev = act_in.shape[0]
        global_rows = per_dev * groups
        spatial = act_in.shape[1] * act_in.shape[2]
        c_mid = act_in.shape[3]
        c_out = shortcut.shape[3]
        classes = w_fc.shape[1]
        dev = lax.axis_index('dp')
        wt, vt = w_fc.T, vel_fc.T
        a3 = act_in.reshape(per_dev, spatial, c_mid).transpose(1, 0, 2)
        s3 = shortcut.reshape(per_dev, spatial, c_out).transpose(1, 0, 2)
        gcw, stats, asum, wb, pooled, y = front(a3, s3, w_conv, bn_gamma, bn_beta)
        p_all = lax.all_gather(pooled, 'dp', tiled=True)
        d_pool, own, loss_part, bias_wide = head_pass(wt, fc_bias, pooled, labels, global_rows, spatial)
        d_conv, d_gamma, d_beta = conv_grad(a3, y, d_pool, stats, gcw, asum, wb)
        own, p_all, d_conv = lax.optimization_barrier((own, p_all, d_conv))
        lr = learn_rate[None]
        grads, p_bf, db, rows_in, rate = shared_grads(groups, wt, bias_wide, p_all, own, lr)
        vec = jnp.concatenate([db.reshape(-1)[:classes], d_gamma[0], d_beta[0], loss_part])
        g_conv, vec = lax.psum((d_conv, vec), 'dp')
        fc_new, fc_vel_new, dep = fused_update(rate, wt, vt, grads, bias_wide, p_bf, rows_in)
        conv_new, conv_vel_new = conv_update(dep, lr, g_conv, w_conv, vel_conv)
        g_bias, g_gamma, g_beta, loss_val = vec[:classes], vec[classes:classes + c_out], vec[classes + c_out:classes + 2 * c_out], vec[classes + 2 * c_out]
        gamma_vel_new = MOMENTUM * vel_gamma + learn_rate * g_gamma
        beta_vel_new = MOMENTUM * vel_beta + learn_rate * g_beta
        bias_vel_new = MOMENTUM * vel_bias + learn_rate * g_bias
        return (conv_new, bn_gamma - gamma_vel_new, bn_beta - beta_vel_new, fc_new.T, fc_bias - bias_vel_new, conv_vel_new, gamma_vel_new, beta_vel_new, fc_vel_new.T, bias_vel_new, loss_val)

    return jax.shard_map(local_step, mesh=mesh, in_specs=(P('dp'),) * 3 + (P(),) * 11, out_specs=(P(),) * 11, check_vma=False)
```

```python
import functools

import jax
import jax.numpy as jnp
from jax import lax
from jax.experimental import pallas as pl
from jax.experimental.pallas import tpu as pltpu
from jax.sharding import PartitionSpec as P

BN_EPS = 1e-5
SMOOTHING = 0.1
MOMENTUM = 0.9
TRUST_COEF = 0.001
WEIGHT_DECAY = 5e-5

TILE = 256
BLK = 32
SLOTS = TILE // BLK
HAVE = 3
NORM = 2
GROUP = 4
CHUNK = 512
POS = 7
WIDTH = 512
LANES = 128
SUB = 8
RING = 4
DEPTH = 3
VMEM_LIMIT = 66_000_000


def aligned(i, size):
    return pl.ds(pl.multiple_of(i, size), size)


def tiled(x, reps):
    return jnp.concatenate([x] * reps, axis=1)


def logit_grads(z, bias, lse, lab, base, classes):
    cols = z.shape[1]
    row = (lax.broadcasted_iota(jnp.int32, (BLK, cols), 0) + base).astype(jnp.float32)
    e = jnp.exp(z + tiled(bias, cols // LANES) - lse)
    low = SMOOTHING / classes
    return e - jnp.where(lab == row, low + (1.0 - SMOOTHING), low)


def grad_kernel(classes, groups, steps, *refs):
    nw = GROUP * HAVE
    ws, biases = refs[:nw], refs[nw:nw + GROUP]
    (p_all, own, lr, g_out, p_out, db_out, rows_out, rate_out, p, pbuf, lhs, dmat, gbuf, meta, sq, msg, msgs,
     p_sem, keep_sem, g_sem, gs_sem, gr_sem, meta_s, meta_r, msg_s, msg_r) = refs[nw + GROUP:]
    me = lax.axis_index('dp')
    q, c = me // 2, me % 2
    step = pl.program_id(0)
    rows_total, feats = p.shape
    per_dev = rows_total // groups

    def slot_of(i):
        return (2 * q + i) % SLOTS

    def base_of(group, k):
        return (2 * (GROUP * group + k // HAVE) + c) * TILE + slot_of(k % HAVE) * BLK

    def prepare(group):
        for k in range(nw):
            valid = lax.broadcasted_iota(jnp.int32, (BLK, feats), 0) < classes - base_of(group, k)
            w = jnp.where(valid, ws[k][...], 0.0)
            if k % HAVE < NORM:
                sq[1] += jnp.sum((w * w).reshape(BLK // 8, 8, feats), axis=0)
            lhs[group % 2, k * BLK:(k + 1) * BLK, :] = w.astype(jnp.bfloat16)

    def local(group):
        return pltpu.make_async_copy(gbuf.at[group % 2], g_out.at[c, pl.ds(group * GROUP, GROUP)], g_sem.at[group % 2])

    def remote(group):
        return pltpu.make_async_remote_copy(
            gbuf.at[group % 2], g_out.at[c, pl.ds(group * GROUP, GROUP)], gs_sem.at[group % 2], gr_sem.at[group],
            device_id=(me + 1 - 2 * c,), device_id_type=pl.DeviceIdType.MESH)

    def arrival(group):
        return pltpu.make_async_remote_copy(
            gbuf.at[group % 2], g_out.at[1 - c, pl.ds(group * GROUP, GROUP)], gs_sem.at[group % 2], gr_sem.at[group],
            device_id=(me + 1 - 2 * c,), device_id_type=pl.DeviceIdType.MESH)

    def spread(src, dst, send, recv):
        return [pltpu.make_async_remote_copy(
            src, dst.at[me], send.at[o], recv.at[o],
            device_id=((me + o) % groups,), device_id_type=pl.DeviceIdType.MESH) for o in range(1, groups)]

    keep = pltpu.make_async_copy(p, p_out, keep_sem)

    @pl.when(step == 0)
    def _():
        def fetch(i):
            return pltpu.make_async_copy(p_all.at[aligned(i * per_dev, per_dev)], pbuf.at[i], p_sem.at[i])

        for i in range(groups):
            fetch(i).start()
        barrier = pltpu.get_barrier_semaphore()
        for o in range(1, groups):
            pl.semaphore_signal(barrier, 1, device_id=((me + o) % groups,), device_id_type=pl.DeviceIdType.MESH)
        pl.semaphore_wait(barrier, groups - 1)
        for copy in spread(own, meta, meta_s, meta_r):
            copy.start()
        meta[me] = own[...]
        sq[...] = jnp.zeros_like(sq)
        prepare(0)

        def convert(i, carry):
            fetch(i).wait()
            p[aligned(i * per_dev, per_dev), :] = pbuf[i].astype(jnp.bfloat16)
            return carry

        lax.fori_loop(0, groups, convert, 0)
        keep.start()
        for copy in spread(own, meta, meta_s, meta_r):
            copy.wait()
        for d in range(groups):
            rows_out[:, d * per_dev:(d + 1) * per_dev] = meta[d]

    @pl.when(step > 1)
    def _():
        local(step - 2).start()
        remote(step - 2).start()

    @pl.when(step > 2)
    def _():
        local(step - 3).wait()
        remote(step - 3).wait_send()

    @pl.when(step > 0)
    def _():
        group = step - 1
        now = group % 2
        prepare(step)
        sums = [jnp.zeros((BLK, LANES), jnp.float32) for _ in range(nw)]
        for n in range(rows_total // CHUNK):
            cs = slice(n * CHUNK, (n + 1) * CHUNK)
            z = lax.dot_general(lhs[now], p[cs, :], (((1,), (1,)), ((), ())), preferred_element_type=jnp.float32)
            for k in range(nw):
                rs = slice(k * BLK, (k + 1) * BLK)
                bias = biases[k // HAVE][aligned(slot_of(k % HAVE) * BLK, BLK), :]
                d = logit_grads(z[rs], bias, rows_out[0:1, cs], rows_out[1:2, cs], base_of(group, k), classes)
                valid = lax.broadcasted_iota(jnp.int32, (BLK, CHUNK), 0) < classes - base_of(group, k)
                d = jnp.where(valid, d, 0.0)
                for m in range(CHUNK // LANES):
                    sums[k] = sums[k] + d[:, m * LANES:(m + 1) * LANES]
                dmat[rs, cs] = d.astype(jnp.bfloat16)
        lane = lax.broadcasted_iota(jnp.int32, (1, TILE), 1)
        db_out[...] = jnp.zeros_like(db_out)
        for t in range(GROUP):
            line = jnp.zeros((1, TILE), jnp.float32)
            for i in range(NORM):
                row = jnp.sum(sums[t * HAVE + i].T, axis=0, keepdims=True)
                line = jnp.where(lane // BLK == slot_of(i), tiled(row, SLOTS), line)
            db_out[0, pl.ds(2 * t + c, 1), :] = line * (1.0 / rows_total)
        for n in range(feats // CHUNK):
            cs = slice(n * CHUNK, (n + 1) * CHUNK)
            g = jnp.dot(dmat[...], p[:, cs], preferred_element_type=jnp.float32) * (1.0 / rows_total)
            for k in range(nw):
                gk = g[k * BLK:(k + 1) * BLK]
                gbuf[now, k // HAVE, (k % HAVE) * BLK:(k % HAVE + 1) * BLK, cs] = gk
                if k % HAVE < NORM:
                    sq[0, :, cs] += jnp.sum((gk * gk).reshape(BLK // 8, 8, CHUNK), axis=0)

    @pl.when(step == steps)
    def _():
        for i in range(2):
            parts = sq[i]
            total = parts[:, 0:LANES]
            for m in range(1, feats // LANES):
                total = total + parts[:, m * LANES:(m + 1) * LANES]
            msg[i] = total
        local(steps - 1).start()
        remote(steps - 1).start()
        keep.wait()
        local(steps - 2).wait()
        remote(steps - 2).wait_send()
        for copy in spread(msg, msgs, msg_s, msg_r):
            copy.start()
        msgs[me] = msg[...]
        local(steps - 1).wait()
        remote(steps - 1).wait_send()
        for group in range(steps):
            arrival(group).wait_recv()
        for copy in spread(msg, msgs, msg_s, msg_r):
            copy.wait()
        both = jnp.sum(msgs[...], axis=0)
        g_norm = jnp.sqrt(jnp.sum(both[0]))
        w_norm = jnp.sqrt(jnp.sum(both[1]))
        rate_out[...] = jnp.full(rate_out.shape, lr[0] * TRUST_COEF * w_norm / (g_norm + WEIGHT_DECAY * w_norm), jnp.float32)


def shared_grads(groups, wt, bias, p_all, own, lr):
    classes, feats = wt.shape
    rows_total = p_all.shape[0]
    n_tiles = pl.cdiv(classes, TILE)
    steps = pl.cdiv(pl.cdiv(n_tiles, 2), GROUP)
    last = pl.cdiv(classes, BLK) - 1

    def w_map(t, i):
        def index(s):
            me = lax.axis_index('dp')
            tile = 2 * (GROUP * jnp.minimum(s, steps - 1) + t) + me % 2
            return jnp.minimum(tile * SLOTS + (2 * (me // 2) + i) % SLOTS, last), 0
        return index

    def b_map(t):
        return lambda s: (jnp.minimum(2 * (GROUP * jnp.maximum(s - 1, 0) + t) + lax.axis_index('dp') % 2, n_tiles - 1), 0)

    rows = GROUP * HAVE * BLK
    anywhere = pl.BlockSpec(memory_space=pl.ANY)
    dma = pltpu.SemaphoreType.DMA
    return pl.pallas_call(
        functools.partial(grad_kernel, classes, groups, steps),
        grid=(steps + 1,),
        in_specs=[pl.BlockSpec((BLK, feats), w_map(t, i)) for t in range(GROUP) for i in range(HAVE)]
        + [pl.BlockSpec((TILE, LANES), b_map(t)) for t in range(GROUP)]
        + [anywhere, pl.BlockSpec(own.shape, lambda s: (0, 0)), pl.BlockSpec(memory_space=pltpu.SMEM)],
        out_specs=[
            anywhere, anywhere,
            pl.BlockSpec((1, 2 * GROUP, TILE), lambda s: (jnp.maximum(s - 1, 0), 0, 0)),
            pl.BlockSpec((8, rows_total), lambda s: (0, 0)),
            pl.BlockSpec((8, LANES), lambda s: (0, 0)),
        ],
        out_shape=[
            jax.ShapeDtypeStruct((2, steps * GROUP, HAVE * BLK, feats), jnp.float32),
            jax.ShapeDtypeStruct((rows_total, feats), jnp.bfloat16),
            jax.ShapeDtypeStruct((steps, 2 * GROUP, TILE), jnp.float32),
            jax.ShapeDtypeStruct((8, rows_total), jnp.float32),
            jax.ShapeDtypeStruct((8, LANES), jnp.float32),
        ],
        scratch_shapes=[
            pltpu.VMEM((rows_total, feats), jnp.bfloat16),
            pltpu.VMEM((groups, rows_total // groups, feats), jnp.float32),
            pltpu.VMEM((2, rows, feats), jnp.bfloat16), pltpu.VMEM((rows, rows_total), jnp.bfloat16),
            pltpu.VMEM((2, GROUP, HAVE * BLK, feats), jnp.float32),
            pltpu.VMEM((groups,) + own.shape, jnp.float32),
            pltpu.VMEM((2, 8, feats), jnp.float32), pltpu.VMEM((2, 8, LANES), jnp.float32), pltpu.VMEM((groups, 2, 8, LANES), jnp.float32),
            dma((groups,)), dma, dma((2,)), dma((2,)), dma((steps,)),
            dma((groups,)), dma((groups,)), dma((groups,)), dma((groups,)),
        ],
        compiler_params=pltpu.CompilerParams(dimension_semantics=("arbitrary",), vmem_limit_bytes=VMEM_LIMIT, collective_id=0, has_side_effects=True),
        cost_estimate=pl.CostEstimate(flops=4 * steps * rows * feats * rows_total, bytes_accessed=8 * steps * rows * feats, transcendentals=0),
        name="shared_grads",
    )(*([wt] * (GROUP * HAVE)), *([bias] * GROUP), p_all, own, lr)


def update_kernel(classes, steps, rate, w_hbm, v_hbm, w_end, v_end, even, odd, bias, p, rows_in, w_out, v_out, done, wbuf, vbuf, lhs, dmat, w_sem, v_sem):
    q = lax.axis_index('dp') // 2
    step = pl.program_id(0)
    a = tiled(rate[0:1, :], CHUNK // LANES)
    cols, feats = p.shape
    small, decay = a * (1.0 / cols), a * WEIGHT_DECAY
    tall = 2 * TILE
    whole = (classes - (steps - 1) * tall) // SUB * SUB
    done[...] = jnp.zeros_like(done)

    def fetch(i, act, hbm, buf, sem):
        slot = lax.rem(i, DEPTH)

        def go(size):
            act(pltpu.make_async_copy(hbm.at[pl.ds(pl.multiple_of(i * tall, tall), size)], buf.at[slot, pl.ds(0, size)], sem.at[slot]))

        @pl.when(i < steps - 1)
        def _():
            go(tall)

        @pl.when(i == steps - 1)
        def _():
            go(whole)

    start = lambda copy: copy.start()
    wait = lambda copy: copy.wait()

    def arrived(i, hbm, buf, sem, end):
        fetch(i, wait, hbm, buf, sem)

        @pl.when(i == steps - 1)
        def _():
            buf[lax.rem(i, DEPTH), whole:whole + SUB, :] = end[...]

    slot = lax.rem(step, DEPTH)

    def apply(rs, cs, g, a):
        w = wbuf[slot, rs, cs]
        nv = MOMENTUM * vbuf[slot, rs, cs] + a * g + decay * w
        v_out[rs, cs] = nv
        w_out[rs, cs] = w - nv

    bases = []
    for t in range(2):
        for i in range(HAVE, SLOTS):
            bases.append(t * TILE + (2 * q + i) % SLOTS * BLK)

    @pl.when(step == 0)
    def _():
        for i in range(2):
            fetch(i, start, w_hbm, wbuf, w_sem)
            fetch(i, start, v_hbm, vbuf, v_sem)

    arrived(step, w_hbm, wbuf, w_sem, w_end)
    arrived(step, v_hbm, vbuf, v_sem, v_end)
    fetch(step + 2, start, w_hbm, wbuf, w_sem)
    fetch(step + 2, start, v_hbm, vbuf, v_sem)
    for k, base in enumerate(bases):
        lhs[k * BLK:(k + 1) * BLK, :] = wbuf[slot, aligned(base, BLK), :].astype(jnp.bfloat16)
    for n in range(cols // CHUNK):
        cs = slice(n * CHUNK, (n + 1) * CHUNK)
        z = lax.dot_general(lhs[...], p[cs, :], (((1,), (1,)), ((), ())), preferred_element_type=jnp.float32)
        for t, src in enumerate((even, odd)):
            for i in range(HAVE):
                apply(aligned(t * TILE + (2 * q + i) % SLOTS * BLK, BLK), cs, src[0, 0, i * BLK:(i + 1) * BLK, cs], a)
        for k, base in enumerate(bases):
            rs = slice(k * BLK, (k + 1) * BLK)
            d = logit_grads(z[rs], bias[aligned(base, BLK), :], rows_in[0:1, cs], rows_in[1:2, cs], step * tall + base, classes)
            dmat[rs, cs] = d.astype(jnp.bfloat16)

    for n in range(feats // CHUNK):
        cs = slice(n * CHUNK, (n + 1) * CHUNK)
        g = jnp.dot(dmat[...], p[:, cs], preferred_element_type=jnp.float32)
        for k, base in enumerate(bases):
            apply(aligned(base, BLK), cs, g[k * BLK:(k + 1) * BLK], small)


def fused_update(rate, wt, vt, grads, bias, p, rows_in):
    classes, feats = wt.shape
    tall = 2 * TILE
    steps = pl.cdiv(classes, tall)
    whole = lambda a: pl.BlockSpec(a.shape, lambda s: (0, 0), pipeline_mode=pl.Buffered(1))
    anywhere = pl.BlockSpec(memory_space=pl.ANY)
    end = pl.BlockSpec((SUB, feats), lambda s: (classes // SUB, 0), pipeline_mode=pl.Buffered(1))
    tile = pl.BlockSpec((tall, feats), lambda s: (s, 0))
    part = lambda par: pl.BlockSpec((1, 1, HAVE * BLK, feats), lambda s: (par, s, 0, 0))
    rows = 2 * (SLOTS - HAVE) * BLK
    dma = pltpu.SemaphoreType.DMA
    return pl.pallas_call(
        functools.partial(update_kernel, classes, steps),
        grid=(steps,),
        in_specs=[whole(rate), anywhere, anywhere, end, end, part(0), part(1), pl.BlockSpec((tall, LANES), lambda s: (s, 0)), whole(p), whole(rows_in)],
        out_specs=[tile, tile, pl.BlockSpec((SUB, LANES), lambda s: (0, 0))],
        scratch_shapes=[
            pltpu.VMEM((DEPTH, tall, feats), jnp.float32), pltpu.VMEM((DEPTH, tall, feats), jnp.float32),
            pltpu.VMEM((rows, feats), jnp.bfloat16), pltpu.VMEM((rows, p.shape[0]), jnp.bfloat16), dma((DEPTH,)), dma((DEPTH,)),
        ],
        out_shape=[jax.ShapeDtypeStruct(wt.shape, jnp.float32)] * 2 + [jax.ShapeDtypeStruct((SUB, LANES), jnp.float32)],
        compiler_params=pltpu.CompilerParams(dimension_semantics=("arbitrary",), vmem_limit_bytes=VMEM_LIMIT),
        cost_estimate=pl.CostEstimate(flops=4 * steps * rows * feats * p.shape[0], bytes_accessed=16 * classes * feats, transcendentals=0),
        name="fused_update",
    )(rate, wt, vt, wt, vt, grads, grads, bias, p, rows_in)


def conv_update_kernel(dep, lr, g_hbm, w_hbm, v_hbm, w_out, v_out, g, w, v, sem, out_sem):
    loads = [pltpu.make_async_copy(x, y, sem.at[i]) for i, (x, y) in enumerate(((g_hbm, g), (w_hbm, w), (v_hbm, v)))]
    for copy in loads:
        copy.start()
    parts = out_sem.shape[1]
    size = g.shape[0] // parts

    def square_sum(ref):
        def add(i, acc):
            x = ref[aligned(i * size, size)]
            return acc + jnp.sum((x * x).reshape(size // SUB, SUB, x.shape[1]), axis=0)
        return jnp.sum(lax.fori_loop(0, parts, add, jnp.zeros((SUB, ref.shape[1]), jnp.float32)))

    loads[0].wait()
    g_norm = jnp.sqrt(square_sum(g))
    loads[1].wait()
    w_norm = jnp.sqrt(square_sum(w))
    loads[2].wait()
    rate = lr[0] * TRUST_COEF * w_norm / (g_norm + WEIGHT_DECAY * w_norm)

    def stores(i):
        at = aligned(i * size, size)
        return [pltpu.make_async_copy(w.at[at], w_out.at[at], out_sem.at[0, i]), pltpu.make_async_copy(v.at[at], v_out.at[at], out_sem.at[1, i])]

    def update(i, carry):
        at = aligned(i * size, size)
        nv = MOMENTUM * v[at] + rate * (g[at] + WEIGHT_DECAY * w[at])
        v[at] = nv
        w[at] = w[at] - nv
        for copy in stores(i):
            copy.start()
        return carry

    def finish(i, carry):
        for copy in stores(i):
            copy.wait()
        return carry

    lax.fori_loop(0, parts, update, 0)
    lax.fori_loop(0, parts, finish, 0)


def conv_update(dep, lr, g, w, v):
    anywhere = pl.BlockSpec(memory_space=pl.ANY)
    dma = pltpu.SemaphoreType.DMA
    return pl.pallas_call(
        conv_update_kernel,
        in_specs=[pl.BlockSpec(memory_space=pltpu.VMEM), pl.BlockSpec(memory_space=pltpu.SMEM), anywhere, anywhere, anywhere],
        out_specs=[anywhere, anywhere],
        out_shape=[jax.ShapeDtypeStruct(w.shape, jnp.float32)] * 2,
        scratch_shapes=[pltpu.VMEM(w.shape, jnp.float32)] * 3 + [dma((3,)), dma((2, 8))],
        compiler_params=pltpu.CompilerParams(vmem_limit_bytes=VMEM_LIMIT),
        cost_estimate=pl.CostEstimate(flops=10 * w.size, bytes_accessed=20 * w.size, transcendentals=0),
        name="conv_update",
    )(dep, lr, g, w, v)


def front_kernel(spatial, scans, chunks, a_hbm, s, wc, gamma, beta, gcw_out, stats_out, asum_out, wb_out, p_out, y_out, a, gram, asum, parts, wb, stats, sem):
    step = pl.program_id(0)
    c_mid = a.shape[-1]
    cols = wc.shape[1]
    pos_count = spatial * a.shape[1]
    wide = 4 * CHUNK

    def fetch(i):
        at = pl.ds(i * POS, POS)
        return pltpu.make_async_copy(a_hbm.at[at], a.at[at], sem.at[i])

    @pl.when(step == 0)
    def _():
        for i in range(scans):
            fetch(i).start()
        gram[...] = jnp.zeros_like(gram)
        asum[...] = jnp.zeros_like(asum)
        p_out[...] = jnp.zeros_like(p_out)

    @pl.when(step < scans)
    def _():
        fetch(step).wait()
        x = a[pl.ds(step * POS, POS)].reshape(-1, c_mid)
        gram[...] += lax.dot_general(x, x, (((0,), (0,)), ((), ())), preferred_element_type=jnp.float32)
        asum[...] += jnp.sum(x.astype(jnp.float32).reshape(-1, SUB, c_mid), axis=0)

    @pl.when(step == scans)
    def _():
        total = jnp.sum(asum[...], axis=0, keepdims=True)
        col = jnp.broadcast_to(total, (LANES, c_mid)).T
        asum_out[...] = col
        rest = gram[...] - tiled(col, c_mid // LANES) * (total / pos_count)
        for i in range(parts.shape[0]):
            part = rest.astype(jnp.bfloat16)
            parts[i] = part
            rest = rest - part.astype(jnp.float32)

    @pl.when(jnp.logical_and(step >= scans, step < scans + chunks))
    def _():
        at = aligned((step - scans) * cols, cols)
        w = wc[...].astype(jnp.bfloat16)
        wb_out[...] = w
        wb[:, at] = w
        wr = w.astype(jnp.float32)
        gcw = jnp.zeros((c_mid, cols), jnp.float32)
        for i in reversed(range(parts.shape[0])):
            gcw = gcw + jnp.dot(parts[i], w, preferred_element_type=jnp.float32)
        gcw_out[...] = gcw
        var = jnp.maximum(jnp.sum(wr * gcw, axis=0, keepdims=True) / pos_count, 0.0)
        mean = jnp.sum(wr * tiled(asum_out[...], cols // LANES), axis=0, keepdims=True) / pos_count
        inv = lax.rsqrt(var + BN_EPS)
        scale = gamma[...] * inv
        rows = (mean, inv, scale, beta[...] - mean * scale)
        rows = jnp.concatenate(rows + (jnp.zeros_like(inv),) * (SUB - len(rows)), axis=0)
        stats_out[...] = rows
        stats[:, at] = rows

    @pl.when(step >= scans + chunks)
    def _():
        first = (step - scans - chunks) * POS

        def chunk(n, carry):
            cs = aligned(n * wide, wide)
            scale, shift = stats[2:3, cs], stats[3:4, cs]
            for j in range(POS):
                z = jnp.dot(a[first + j], wb[:, cs], preferred_element_type=jnp.float32)
                y = jnp.maximum(z * scale + shift + s[j, :, cs].astype(jnp.float32), 0.0)
                y_out[j, :, cs] = y.astype(jnp.bfloat16)
                p_out[:, cs] += y
            return carry

        lax.fori_loop(0, p_out.shape[1] // wide, chunk, 0)

    @pl.when(step == pl.num_programs(0) - 1)
    def _():
        p_out[...] = p_out[...] * (1.0 / spatial)


def front(a3, s3, w_conv, gamma, beta):
    spatial, per_dev, c_mid = a3.shape
    c_out = w_conv.shape[1]
    scans, chunks = spatial // POS, c_out // CHUNK
    fixed = lambda shape: pl.BlockSpec(shape, lambda i: (0, 0))
    chunk = lambda rows: pl.BlockSpec((rows, CHUNK), lambda i: (0, jnp.clip(i - scans, 0, chunks - 1)))
    part = pl.BlockSpec((POS, per_dev, c_out), lambda i: (jnp.maximum(i - scans - chunks, 0), 0, 0))
    return pl.pallas_call(
        functools.partial(front_kernel, spatial, scans, chunks),
        grid=(2 * scans + chunks,),
        in_specs=[pl.BlockSpec(memory_space=pl.ANY), part, chunk(c_mid), chunk(1), chunk(1)],
        out_specs=[chunk(c_mid), chunk(SUB), fixed((c_mid, LANES)), chunk(c_mid), fixed((per_dev, c_out)), part],
        out_shape=[
            jax.ShapeDtypeStruct((c_mid, c_out), jnp.float32),
            jax.ShapeDtypeStruct((SUB, c_out), jnp.float32),
            jax.ShapeDtypeStruct((c_mid, LANES), jnp.float32),
            jax.ShapeDtypeStruct((c_mid, c_out), jnp.bfloat16),
            jax.ShapeDtypeStruct((per_dev, c_out), jnp.float32),
            jax.ShapeDtypeStruct((spatial, per_dev, c_out), jnp.bfloat16),
        ],
        scratch_shapes=[
            pltpu.VMEM(a3.shape, jnp.bfloat16), pltpu.VMEM((c_mid, c_mid), jnp.float32), pltpu.VMEM((SUB, c_mid), jnp.float32),
            pltpu.VMEM((3, c_mid, c_mid), jnp.bfloat16), pltpu.VMEM((c_mid, c_out), jnp.bfloat16), pltpu.VMEM((SUB, c_out), jnp.float32),
            pltpu.SemaphoreType.DMA((scans,)),
        ],
        compiler_params=pltpu.CompilerParams(dimension_semantics=("arbitrary",), vmem_limit_bytes=VMEM_LIMIT),
        cost_estimate=pl.CostEstimate(flops=2 * spatial * per_dev * c_mid * (c_mid + c_out), bytes_accessed=4 * spatial * per_dev * c_out, transcendentals=0),
        name="front",
    )(a3, s3, w_conv, gamma[None, :], beta[None, :])


def head_kernel(classes, global_rows, spatial, tiles, bsum, lab_s, w_hbm, tail, bias, p, lab, dpool_out, own_out, loss_out, wide_out, pt, wb, zb, acc, wsum, top, tot, ly, ring, wy, sem, row_sem):
    step = pl.program_id(0)
    rows, feats = p.shape
    width = ring.shape[1]
    now, prev = lax.rem(step, 2), lax.rem(step + 1, 2)
    left = classes - (tiles - 1) * width

    def fetch(i):
        slot = lax.rem(i, RING)
        return pltpu.make_async_copy(w_hbm.at[aligned(i * width, width)], ring.at[slot], sem.at[slot])

    def pick(i):
        return pltpu.make_async_copy(w_hbm.at[pl.ds(lab_s[i], 1)], wy.at[pl.ds(i, 1)], row_sem)

    def column(x):
        return jnp.broadcast_to(x, (LANES, rows)).T

    def logits(w):
        wb[now] = w
        b = jnp.broadcast_to(bias[...], (LANES, width)).T
        wide_out[...] = b
        half = width // 2
        for h in range(2):
            at = slice(h * half, (h + 1) * half)
            zb[now, at] = jnp.dot(w[at], pt[...], preferred_element_type=jnp.float32) + tiled(b[at], rows // LANES)

    @pl.when(step == 0)
    def _():
        for i in range(RING - 1):
            fetch(i).start()

        def begin(i, carry):
            pick(i).start()
            return carry

        lax.fori_loop(0, rows, begin, 0)
        pt[...] = p[...].astype(jnp.bfloat16).T
        acc[...] = jnp.zeros_like(acc)
        wsum[...] = jnp.zeros_like(wsum)
        top[...] = jnp.full_like(top, -1e30)
        tot[...] = jnp.zeros_like(tot)
        ly[...] = jnp.zeros_like(ly)
        row = lax.broadcasted_iota(jnp.int32, (width, feats), 0)
        logits(jnp.where(row < left, tail[...], 0.0).astype(jnp.bfloat16))
        row = lax.broadcasted_iota(jnp.int32, (width, rows), 0)
        zb[now] = jnp.where(row < left, zb[now], -1e30)

    @pl.when(jnp.logical_and(step > 0, step < tiles))
    def _():
        fetch(step - 1).wait()

    @pl.when(jnp.logical_and(step > 0, step + RING - 2 < tiles - 1))
    def _():
        fetch(step + RING - 2).start()

    @pl.when(step > 0)
    def _():
        z = zb[prev]
        old = top[...]
        new = jnp.maximum(old, jnp.max(z, axis=0, keepdims=True))
        corr = jnp.exp(old - new)
        e = jnp.exp(z - new)
        top[...] = new
        tot[...] = tot[...] * corr + jnp.sum(e, axis=0, keepdims=True)
        base = jnp.where(step == 1, tiles - 1, step - 2) * width
        row = lax.broadcasted_iota(jnp.int32, (width, rows), 0) + base
        ly[...] += jnp.sum(jnp.where(lab[...] == row, z, 0.0), axis=0, keepdims=True)
        lead = jnp.concatenate([e.astype(jnp.bfloat16).T, jnp.ones((16, width), jnp.bfloat16)], axis=0)
        wide_corr = column(corr)
        logits(ring[lax.rem(step + RING - 1, RING)].astype(jnp.bfloat16))
        for n in range(feats // CHUNK):
            cs = slice(n * CHUNK, (n + 1) * CHUNK)
            part = jnp.dot(lead, wb[prev, :, cs], preferred_element_type=jnp.float32)
            acc[:, cs] = acc[:, cs] * tiled(wide_corr, CHUNK // LANES) + part[:rows]
            wsum[:, cs] += part[rows:rows + 8]

    @pl.when(step == tiles)
    def _():
        pltpu.make_async_copy(w_hbm.at[pl.ds(0, rows)], wy, row_sem).wait()
        lse = top[...] + jnp.log(tot[...])
        ws = wsum[0:1, :]
        lsum = jnp.sum(pt[...].astype(jnp.float32) * tiled(jnp.broadcast_to(ws, (LANES, feats)).T, rows // LANES), axis=0, keepdims=True) + bsum[0]
        own_out[...] = jnp.concatenate([lse, lab[...].astype(jnp.float32)] + [jnp.zeros_like(lse)] * 6, axis=0)
        loss = lse - (1.0 - SMOOTHING) * ly[...] - SMOOTHING / classes * lsum
        loss_out[0] = jnp.sum(loss) * (1.0 / global_rows)
        d = acc[...] / tiled(column(tot[...]), feats // LANES) - (1.0 - SMOOTHING) * wy[...] - SMOOTHING / classes * ws
        dpool_out[...] = d * (1.0 / (global_rows * spatial))


def head_pass(wt, bias, p, lab, global_rows, spatial):
    classes, feats = wt.shape
    rows = p.shape[0]
    tiles = pl.cdiv(classes, WIDTH)
    fixed = lambda shape: pl.BlockSpec(shape, lambda i: (0,) * len(shape), pipeline_mode=pl.Buffered(1))
    kept = lambda shape: pl.BlockSpec(shape, lambda i: (0,) * len(shape))
    line = (1, rows)
    order = lambda i: jnp.where(i == 0, tiles - 1, jnp.minimum(i - 1, tiles - 2))
    return pl.pallas_call(
        functools.partial(head_kernel, classes, global_rows, spatial, tiles),
        grid=(tiles + 1,),
        in_specs=[
            pl.BlockSpec(memory_space=pltpu.SMEM),
            pl.BlockSpec(memory_space=pltpu.SMEM),
            pl.BlockSpec(memory_space=pl.ANY),
            pl.BlockSpec((WIDTH, feats), lambda i: (tiles - 1, 0), pipeline_mode=pl.Buffered(1)),
            pl.BlockSpec((1, WIDTH), lambda i: (0, order(i))),
            fixed(p.shape), fixed(line),
        ],
        out_specs=[kept(p.shape), kept((8, rows)), pl.BlockSpec(memory_space=pltpu.SMEM), pl.BlockSpec((WIDTH, LANES), lambda i: (order(i), 0))],
        out_shape=[
            jax.ShapeDtypeStruct(p.shape, jnp.float32),
            jax.ShapeDtypeStruct((8, rows), jnp.float32),
            jax.ShapeDtypeStruct((1,), jnp.float32),
            jax.ShapeDtypeStruct((tiles * WIDTH, LANES), jnp.float32),
        ],
        scratch_shapes=[
            pltpu.VMEM((feats, rows), jnp.bfloat16), pltpu.VMEM((2, WIDTH, feats), jnp.bfloat16), pltpu.VMEM((2, WIDTH, rows), jnp.float32),
            pltpu.VMEM(p.shape, jnp.float32), pltpu.VMEM((8, feats), jnp.float32),
        ] + [pltpu.VMEM(line, jnp.float32)] * 3 + [pltpu.VMEM((RING, WIDTH, feats), jnp.float32), pltpu.VMEM(p.shape, jnp.float32), pltpu.SemaphoreType.DMA((RING,)), pltpu.SemaphoreType.DMA],
        compiler_params=pltpu.CompilerParams(dimension_semantics=("arbitrary",), vmem_limit_bytes=VMEM_LIMIT),
        cost_estimate=pl.CostEstimate(flops=4 * rows * feats * classes, bytes_accessed=4 * classes * feats, transcendentals=0),
        name="head_pass",
    )(jnp.sum(bias)[None], lab, wt, wt, bias[None, :], p, lab[None, :])


def conv_grad_kernel(pos_count, a, y, dpool, stats, asum, gcw_hbm, wb_hbm, dconv_out, dgamma_out, dbeta_out, db, n_on, gcw, wb, sem):
    step = pl.program_id(0)
    c_mid = a.shape[-1]
    c_out = dpool.shape[1]
    late = [pltpu.make_async_copy(gcw_hbm, gcw, sem.at[0]), pltpu.make_async_copy(wb_hbm, wb, sem.at[1])]

    @pl.when(step == 0)
    def _():
        for copy in late:
            copy.start()
        db[...] = dpool[...].astype(jnp.bfloat16)
        dconv_out[...] = jnp.zeros_like(dconv_out)
        n_on[...] = jnp.zeros_like(n_on)

    x = a[...].reshape(-1, c_mid)
    for n in range(c_out // CHUNK):
        cs = slice(n * CHUNK, (n + 1) * CHUNK)
        on = y[:, :, cs] > 0
        ones = jnp.where(on, jnp.bfloat16(1), jnp.bfloat16(0))
        count = ones[0]
        for j in range(1, POS):
            count = count + ones[j]
        n_on[:, cs] += count
        d = (ones * db[:, cs][None]).reshape(-1, CHUNK)
        dconv_out[:, cs] += lax.dot_general(x, d, (((0,), (0,)), ((), ())), preferred_element_type=jnp.float32)

    @pl.when(step == pl.num_programs(0) - 1)
    def _():
        for copy in late:
            copy.wait()

        def finish(n, carry):
            cs = aligned(n * CHUNK, CHUNK)
            mean, inv, scale = stats[0:1, cs], stats[1:2, cs], stats[2:3, cs]
            count = n_on[:, cs].astype(jnp.float32)
            dbeta_out[:, cs] = jnp.sum(dpool[:, cs] * count, axis=0, keepdims=True)
            dbeta = jnp.sum(db[:, cs].astype(jnp.float32) * count, axis=0, keepdims=True)
            m = dconv_out[:, cs]
            dgamma = inv * (jnp.sum(m * wb[:, cs].astype(jnp.float32), axis=0, keepdims=True) - mean * dbeta)
            dgamma_out[:, cs] = dgamma
            lead = tiled(asum[...], CHUNK // LANES)
            dconv_out[:, cs] = scale * (m - lead * (dbeta / pos_count) - gcw[:, cs] * (inv * dgamma / pos_count))
            return carry

        lax.fori_loop(0, c_out // CHUNK, finish, 0)


def conv_grad(a3, y, dpool, stats, gcw, asum, wb):
    spatial, per_dev, c_mid = a3.shape
    c_out = wb.shape[1]
    pos_count = spatial * per_dev
    fixed = lambda a: pl.BlockSpec(a.shape, lambda i: (0, 0), pipeline_mode=pl.Buffered(1))
    part = lambda width: pl.BlockSpec((POS, per_dev, width), lambda i: (i, 0, 0))
    anywhere = pl.BlockSpec(memory_space=pl.ANY)
    kept = lambda rows: pl.BlockSpec((rows, c_out), lambda i: (0, 0))
    return pl.pallas_call(
        functools.partial(conv_grad_kernel, pos_count),
        grid=(spatial // POS,),
        in_specs=[part(c_mid), part(c_out), fixed(dpool), fixed(stats), fixed(asum), anywhere, anywhere],
        out_specs=[kept(c_mid), kept(1), kept(1)],
        out_shape=[jax.ShapeDtypeStruct((rows, c_out), jnp.float32) for rows in (c_mid, 1, 1)],
        scratch_shapes=[pltpu.VMEM(dpool.shape, jnp.bfloat16), pltpu.VMEM(dpool.shape, jnp.bfloat16), pltpu.VMEM(gcw.shape, jnp.float32), pltpu.VMEM(wb.shape, jnp.bfloat16), pltpu.SemaphoreType.DMA((2,))],
        compiler_params=pltpu.CompilerParams(dimension_semantics=("arbitrary",), vmem_limit_bytes=VMEM_LIMIT),
        cost_estimate=pl.CostEstimate(flops=2 * pos_count * c_mid * c_out, bytes_accessed=2 * pos_count * c_out, transcendentals=0),
        name="conv_grad",
    )(a3, y, dpool, stats, asum, gcw, wb)


def solution(mesh):
    groups = mesh.shape['dp']

    def local_step(act_in, shortcut, labels, w_conv, bn_gamma, bn_beta, w_fc, fc_bias, vel_conv, vel_gamma, vel_beta, vel_fc, vel_bias, learn_rate):
        per_dev = act_in.shape[0]
        global_rows = per_dev * groups
        spatial = act_in.shape[1] * act_in.shape[2]
        c_mid = act_in.shape[3]
        c_out = shortcut.shape[3]
        classes = w_fc.shape[1]
        dev = lax.axis_index('dp')
        wt, vt = w_fc.T, vel_fc.T
        a3 = act_in.reshape(per_dev, spatial, c_mid).transpose(1, 0, 2)
        s3 = shortcut.reshape(per_dev, spatial, c_out).transpose(1, 0, 2)
        gcw, stats, asum, wb, pooled, y = front(a3, s3, w_conv, bn_gamma, bn_beta)
        p_all = lax.all_gather(pooled, 'dp', tiled=True)
        d_pool, own, loss_part, bias_wide = head_pass(wt, fc_bias, pooled, labels, global_rows, spatial)
        d_conv, d_gamma, d_beta = conv_grad(a3, y, d_pool, stats, gcw, asum, wb)
        own, p_all, d_conv = lax.optimization_barrier((own, p_all, d_conv))
        lr = learn_rate[None]
        grads, p_bf, db, rows_in, rate = shared_grads(groups, wt, bias_wide, p_all, own, lr)
        vec = jnp.concatenate([db.reshape(-1)[:classes], d_gamma[0], d_beta[0], loss_part])
        g_conv, vec = lax.psum((d_conv, vec), 'dp')
        fc_new, fc_vel_new, dep = fused_update(rate, wt, vt, grads, bias_wide, p_bf, rows_in)
        conv_new, conv_vel_new = conv_update(dep, lr, g_conv, w_conv, vel_conv)
        g_bias, g_gamma, g_beta, loss_val = vec[:classes], vec[classes:classes + c_out], vec[classes + c_out:classes + 2 * c_out], vec[classes + 2 * c_out]
        gamma_vel_new = MOMENTUM * vel_gamma + learn_rate * g_gamma
        beta_vel_new = MOMENTUM * vel_beta + learn_rate * g_beta
        bias_vel_new = MOMENTUM * vel_bias + learn_rate * g_bias
        return (conv_new, bn_gamma - gamma_vel_new, bn_beta - beta_vel_new, fc_new.T, fc_bias - bias_vel_new, conv_vel_new, gamma_vel_new, beta_vel_new, fc_vel_new.T, bias_vel_new, loss_val)

    return jax.shard_map(local_step, mesh=mesh, in_specs=(P('dp'),) * 3 + (P(),) * 11, out_specs=(P(),) * 11, check_vma=False)
```
